32 devices in a mesh: batch: 2 (over x), col: 4 (over z), row: 4 (over y, core).
Axes of the slice: x: 2, y: 2, z: 4, core: 2. Of those that a mesh axis runs over, the one named last changes fastest.
Arguments:
- mat_blocks: float32 [32768, 128, 32], P(('batch', 'row'), 'col'), parts along dimension 0
Outputs:
- output 1: float32 [32768, 128, 32], P(('batch', 'row'), 'col'), parts along dimension 0
- output 2: float32 [256], P('batch'), parts along dimension 0
- output 3: float32 [8, 32, 32], P('batch'), parts along dimension 0
There are 2 independent parts. The reference program is written for one: setup_inputs(seed, part) draws one part's arguments, and reference() takes and returns one part's arrays. A program takes and returns all parts, laid end to end along the dimension named above; each array names one.
All inputs are finite; a program needn't handle non-finite values.
Results may differ from the reference program's by a relative error of at most 0.001.
Values sent between devices are 32-bit elements.
A program may use at most 1 GiB of HBM per device.

```python
import math
import jax
import jax.numpy as jnp
from jax import lax

MATRIX_ROWS = 16384
MATRIX_COLS = 4096
BLOCK_COLS = 32
PANELS = 4
COL_PROCS = 4
PANEL_COLS = PANELS * BLOCK_COLS
TOTAL_BLOCKS = MATRIX_COLS // BLOCK_COLS
LOCAL_BLOCKS = TOTAL_BLOCKS // COL_PROCS
HIGHEST = lax.Precision.HIGHEST


def mat_dot(left_mat, right_mat):
    return jnp.dot(left_mat, right_mat, precision=HIGHEST, preferred_element_type=jnp.float32)


def to_stored(glob_mat):
    split_mat = glob_mat.reshape(MATRIX_ROWS, LOCAL_BLOCKS, COL_PROCS, BLOCK_COLS)
    return split_mat.transpose(0, 2, 1, 3).reshape(MATRIX_ROWS, TOTAL_BLOCKS, BLOCK_COLS)


def to_global(stored_mat):
    split_mat = stored_mat.reshape(MATRIX_ROWS, COL_PROCS, LOCAL_BLOCKS, BLOCK_COLS)
    return split_mat.transpose(0, 2, 1, 3).reshape(MATRIX_ROWS, MATRIX_COLS)


def setup_inputs(seed: int = 0, part: int = 0) -> dict:
    base_key = jax.random.fold_in(jax.random.key(seed), part)
    key_gauss, key_left, key_right, key_sign = jax.random.split(base_key, 4)
    gauss_part = jax.random.normal(key_gauss, (MATRIX_ROWS, MATRIX_COLS), jnp.float32)
    low_left = jax.random.normal(key_left, (MATRIX_ROWS, 4), jnp.float32)
    low_right = 0.35 * jax.random.normal(key_right, (4, MATRIX_COLS), jnp.float32)
    pivot_sign = 2.0 * jax.random.randint(key_sign, (PANEL_COLS,), 0, 2).astype(jnp.float32) - 1.0
    dense_mat = gauss_part + mat_dot(low_left, low_right)
    diag_ids = jnp.arange(PANEL_COLS)
    dense_mat = dense_mat.at[diag_ids, diag_ids].add(1.2 * math.sqrt(MATRIX_ROWS) * pivot_sign)
    return {'mat_blocks': to_stored(dense_mat)}


def factor_panel(panel_in, pivot_base):
    row_ids = jnp.arange(MATRIX_ROWS)
    col_ids = jnp.arange(BLOCK_COLS)

    def column_step(col_idx, loop_state):
        panel_work, tau_vec = loop_state
        pivot_row = pivot_base + col_idx
        column = lax.dynamic_index_in_dim(panel_work, col_idx, axis=1, keepdims=False)
        alpha_val = lax.dynamic_index_in_dim(column, pivot_row, keepdims=False)
        sub_col = jnp.where(row_ids > pivot_row, column, 0.0)
        norm_val = jnp.sqrt(alpha_val * alpha_val + jnp.sum(sub_col * sub_col))
        beta_val = jnp.where(alpha_val >= 0.0, -norm_val, norm_val)
        tau_val = (beta_val - alpha_val) / beta_val
        refl_vec = sub_col / (alpha_val - beta_val) + jnp.where(row_ids == pivot_row, 1.0, 0.0)
        refl_dot = mat_dot(refl_vec[None, :], panel_work)[0]
        refl_dot = jnp.where(col_ids > col_idx, refl_dot, 0.0)
        new_col = jnp.where(row_ids < pivot_row, column, jnp.where(row_ids == pivot_row, beta_val, refl_vec))
        panel_work = panel_work - tau_val * refl_vec[:, None] * refl_dot[None, :]
        panel_work = jnp.where(col_ids[None, :] == col_idx, new_col[:, None], panel_work)
        tau_vec = jnp.where(col_ids == col_idx, tau_val, tau_vec)
        return panel_work, tau_vec

    return lax.fori_loop(0, BLOCK_COLS, column_step, (panel_in, jnp.zeros((BLOCK_COLS,), jnp.float32)))


def form_tfactor(refl_mat, tau_vec):
    gram_mat = mat_dot(refl_mat.T, refl_mat)
    col_ids = jnp.arange(BLOCK_COLS)

    def tcol_step(col_idx, t_factor):
        gram_col = lax.dynamic_index_in_dim(gram_mat, col_idx, axis=1, keepdims=False)
        tau_val = lax.dynamic_index_in_dim(tau_vec, col_idx, keepdims=False)
        gram_col = jnp.where(col_ids < col_idx, gram_col, 0.0)
        new_col = -tau_val * mat_dot(t_factor, gram_col[:, None])[:, 0]
        new_col = jnp.where(col_ids == col_idx, tau_val, new_col)
        return jnp.where(col_ids[None, :] == col_idx, new_col[:, None], t_factor)

    return lax.fori_loop(0, BLOCK_COLS, tcol_step, jnp.zeros((BLOCK_COLS, BLOCK_COLS), jnp.float32))


def reference(mat_blocks):
    glob_mat = to_global(mat_blocks)
    row_ids = jnp.arange(MATRIX_ROWS)
    col_ids = jnp.arange(BLOCK_COLS)
    tau_list = []
    tfac_list = []
    for panel_idx in range(PANELS):
        col_start = panel_idx * BLOCK_COLS
        col_end = col_start + BLOCK_COLS
        panel_out, tau_vec = factor_panel(glob_mat[:, col_start:col_end], col_start)
        pivot_ids = col_start + col_ids
        refl_mat = jnp.where(row_ids[:, None] > pivot_ids[None, :], panel_out, jnp.where(row_ids[:, None] == pivot_ids[None, :], 1.0, 0.0))
        t_factor = form_tfactor(refl_mat, tau_vec)
        trail_mat = glob_mat[:, col_end:]
        w_mat = mat_dot(t_factor.T, mat_dot(refl_mat.T, trail_mat))
        trail_mat = trail_mat - mat_dot(refl_mat, w_mat)
        glob_mat = jnp.concatenate([glob_mat[:, :col_start], panel_out, trail_mat], axis=1)
        tau_list.append(tau_vec)
        tfac_list.append(t_factor)
    return to_stored(glob_mat), jnp.concatenate(tau_list), jnp.stack(tfac_list)
```

```python
import functools
import jax
import jax.numpy as jnp
from jax import lax
from jax.experimental import pallas as pl
from jax.experimental.pallas import tpu as pltpu
from jax.sharding import PartitionSpec as P

PANELS = 4
BW = 32
NC = PANELS * BW
HIGHEST = lax.Precision.HIGHEST


def dot_nn(x, y):
    return lax.dot_general(x, y, (((1,), (0,)), ((), ())), precision=HIGHEST, preferred_element_type=jnp.float32)


def dot_nt(x, y):
    return lax.dot_general(x, y, (((1,), (1,)), ((), ())), precision=HIGHEST, preferred_element_type=jnp.float32)


def dot_tn(x, y):
    return lax.dot_general(x, y, (((0,), (0,)), ((), ())), precision=HIGHEST, preferred_element_type=jnp.float32)


def factor_kernel(g_ref, b_ref, face_ref, tfull_ref, tau_ref, rit_ref, nmat_ref, uit_ref, u_ref, li_ref):
    nt = NC // 8
    lane = lax.broadcasted_iota(jnp.int32, (8, NC), 1)
    sub = lax.broadcasted_iota(jnp.int32, (8, NC), 0)

    def row_of(tile, s):
        return jnp.broadcast_to(tile[s:s + 1, :], (8, NC))

    def col_of(tile, k):
        return jnp.broadcast_to(tile[:, k:k + 1], (8, NC))

    g = [g_ref[8 * t:8 * t + 8, :] for t in range(nt)]
    b = [b_ref[8 * t:8 * t + 8, :] for t in range(nt)]
    ri = [jnp.where(lane == sub + 8 * t, 1.0, 0.0) for t in range(nt)]
    li = [jnp.where(lane == sub + 8 * t, 1.0, 0.0) for t in range(nt)]
    inv_row = jnp.zeros((8, NC), jnp.float32)
    tau_row = jnp.zeros((8, NC), jnp.float32)
    invs = []
    for k in range(NC):
        t0, s = divmod(k, 8)
        gcol = [col_of(g[t], k) for t in range(t0, nt)]
        bcol = [col_of(b[t], k) for t in range(t0, nt)]
        diag = row_of(gcol[0], s)
        rs = lax.rsqrt(diag)
        rrow = jnp.where(lane >= k, row_of(g[t0], s) * rs, 0.0)
        rirow = row_of(ri[t0], s) * rs
        for t in range(t0, nt):
            f = gcol[t - t0] * rs
            g[t] = g[t] - f * rrow
            ri[t] = ri[t] - f * rirow
        norm = diag * rs
        alpha = row_of(bcol[0], s)
        sgn = jnp.where(alpha >= 0.0, 1.0, -1.0)
        beta = -sgn * norm
        rsig = -sgn * rrow
        brow = row_of(b[t0], s)
        urow = jnp.where(lane >= k, brow - rsig, 0.0)
        piv = alpha - beta
        inv = 1.0 / piv
        tau_row = jnp.where(lane == k, (beta - alpha) / beta, tau_row)
        lrow = brow * inv_row
        inv_row = jnp.where(lane == k, inv, inv_row)
        uupd = jnp.where(lane > k, urow, 0.0)
        lirow = row_of(li[t0], s)
        for t in range(t0, nt):
            f = bcol[t - t0] * inv
            b[t] = b[t] - f * uupd
            li[t] = li[t] - f * lirow
        face_ref[k:k + 1, :] = jnp.where(lane >= k, rsig, lrow)[0:1]
        u_ref[k:k + 1, :] = urow[0:1]
        rit_ref[k:k + 1, :] = (-sgn * rirow)[0:1]
        li_ref[k:k + 1, :] = lirow[0:1]
        invs.append(inv)
    tau_ref[...] = tau_row
    umat = u_ref[...]
    ut = umat.T
    u_t = [ut[8 * t:8 * t + 8, :] for t in range(nt)]
    e = [jnp.where(lane == sub + 8 * t, 1.0, 0.0) for t in range(nt)]
    for k in range(NC):
        t0, s = divmod(k, 8)
        yrow = row_of(e[t0], s) * invs[k]
        uit_ref[k:k + 1, :] = yrow[0:1]
        for t in range(t0, nt):
            e[t] = e[t] - col_of(u_t[t], k) * yrow
    limat = li_ref[...]
    nmat_ref[...] = dot_tn(limat, uit_ref[...])
    tful = -dot_nt(dot_nt(umat, rit_ref[...]), limat)
    rows = lax.broadcasted_iota(jnp.int32, (NC, NC), 0)
    cols = lax.broadcasted_iota(jnp.int32, (NC, NC), 1)
    tful = jnp.where(cols > rows, tful, 0.0)
    tfull_ref[...] = jnp.where(cols == rows, jnp.broadcast_to(tau_row[0:1], (NC, NC)), tful)


def factor(gram, top):
    sq = jax.ShapeDtypeStruct((NC, NC), jnp.float32)
    return pl.pallas_call(
        factor_kernel,
        out_shape=(sq, sq, jax.ShapeDtypeStruct((8, NC), jnp.float32), sq, sq, sq),
        in_specs=[pl.BlockSpec(memory_space=pltpu.VMEM)] * 2,
        out_specs=tuple([pl.BlockSpec(memory_space=pltpu.VMEM)] * 6),
        scratch_shapes=[pltpu.VMEM((NC, NC), jnp.float32), pltpu.VMEM((NC, NC), jnp.float32)],
        name="factor",
    )(gram, top)


def solution(mesh):
    block_spec = P(('batch', 'row'), 'col', None)

    def device_fn(a_local):
        local_rows, local_blocks, bw = a_local.shape
        ncol = local_blocks * bw
        at = a_local.transpose(1, 2, 0).reshape(ncol, local_rows)
        col_rank = lax.axis_index('col')
        row_rank = lax.axis_index('row')
        pt = lax.all_gather(at[:bw], 'col', axis=0, tiled=True)
        xt = dot_nt(at, pt)
        gram = dot_nt(pt, pt)
        head = jnp.where(row_rank == 0, at[:, :NC], 0.0)
        phead = jnp.where(row_rank == 0, pt[:, :NC].T, 0.0)
        packed = lax.psum(jnp.concatenate([xt, head, gram, phead], axis=0), 'row')
        xt = packed[:ncol]
        head = packed[ncol:2 * ncol]
        gram = packed[2 * ncol:2 * ncol + NC]
        phead = packed[2 * ncol + NC:]
        face, tfull, tau8, rit, nmat, uit = factor(gram, phead)
        r12t = dot_nt(xt, rit)
        zt = dot_nn(head - r12t, nmat)
        own = lax.dynamic_slice_in_dim(uit, col_rank * bw, bw, axis=0) if False else None
        uinv_own = lax.dynamic_slice_in_dim(uit.T, col_rank * bw, bw, axis=1).T
        zt = jnp.concatenate([-uinv_own, zt[bw:]], axis=0)
        base = jnp.concatenate([jnp.zeros_like(at[:bw]), at[bw:]], axis=0)
        out = base - dot_nn(zt, pt)
        face_own = lax.dynamic_slice_in_dim(face, col_rank * bw, bw, axis=1).T
        top = jnp.concatenate([face_own, r12t[bw:]], axis=0)
        top = jnp.where(row_rank == 0, top, out[:, :NC])
        out = lax.dynamic_update_slice(out, top, (0, 0))
        a_out = out.reshape(local_blocks, bw, local_rows).transpose(2, 0, 1)
        tfac = jnp.stack([tfull[j * bw:(j + 1) * bw, j * bw:(j + 1) * bw] for j in range(PANELS)])
        return a_out, tau8[0], tfac

    return jax.shard_map(device_fn, mesh=mesh, in_specs=(block_spec,), out_specs=(block_spec, P('batch'), P('batch', None, None)), check_vma=False)
```

```python
import functools
import jax
import jax.numpy as jnp
from jax import lax
from jax.experimental import pallas as pl
from jax.experimental.pallas import tpu as pltpu
from jax.sharding import PartitionSpec as P

PANELS = 4
BW = 32
NC = PANELS * BW
CH = 512
HIGHEST = lax.Precision.HIGHEST
MESH = pl.DeviceIdType.MESH


def dot_nn(x, y):
    return lax.dot_general(x, y, (((1,), (0,)), ((), ())), precision=HIGHEST, preferred_element_type=jnp.float32)


def dot_nt(x, y):
    return lax.dot_general(x, y, (((1,), (1,)), ((), ())), precision=HIGHEST, preferred_element_type=jnp.float32)


def dot_tn(x, y):
    return lax.dot_general(x, y, (((0,), (0,)), ((), ())), precision=HIGHEST, preferred_element_type=jnp.float32)


def factor_kernel(g_ref, ptop_ref, facet_ref, tfac_ref, tau_ref, rit_ref, nmat_ref, uit_ref, u_ref, li_ref, face_ref):
    nt = NC // 8
    lane = lax.broadcasted_iota(jnp.int32, (8, NC), 1)
    sub = lax.broadcasted_iota(jnp.int32, (8, NC), 0)

    def row_of(tile, s):
        return jnp.broadcast_to(tile[s:s + 1, :], (8, NC))

    def col_of(tile, k):
        return jnp.broadcast_to(tile[:, k:k + 1], (8, NC))

    g = [g_ref[8 * t:8 * t + 8, :] for t in range(nt)]
    top = ptop_ref[...].T
    b = [top[8 * t:8 * t + 8, :] for t in range(nt)]
    ri = [jnp.where(lane == sub + 8 * t, 1.0, 0.0) for t in range(nt)]
    li = [jnp.where(lane == sub + 8 * t, 1.0, 0.0) for t in range(nt)]
    inv_row = jnp.zeros((8, NC), jnp.float32)
    tau_row = jnp.zeros((8, NC), jnp.float32)
    invs = []
    for k in range(NC):
        t0, s = divmod(k, 8)
        gcol = [col_of(g[t], k) for t in range(t0, nt)]
        bcol = [col_of(b[t], k) for t in range(t0, nt)]
        diag = row_of(gcol[0], s)
        rs = lax.rsqrt(diag)
        rrow = jnp.where(lane >= k, row_of(g[t0], s) * rs, 0.0)
        rirow = row_of(ri[t0], s) * rs
        for t in range(t0, nt):
            f = gcol[t - t0] * rs
            g[t] = g[t] - f * rrow
            ri[t] = ri[t] - f * rirow
        norm = diag * rs
        alpha = row_of(bcol[0], s)
        sgn = jnp.where(alpha >= 0.0, 1.0, -1.0)
        beta = -sgn * norm
        rsig = -sgn * rrow
        brow = row_of(b[t0], s)
        urow = jnp.where(lane >= k, brow - rsig, 0.0)
        piv = alpha - beta
        inv = 1.0 / piv
        tau_row = jnp.where(lane == k, (beta - alpha) / beta, tau_row)
        lrow = brow * inv_row
        inv_row = jnp.where(lane == k, inv, inv_row)
        uupd = jnp.where(lane > k, urow, 0.0)
        lirow = row_of(li[t0], s)
        for t in range(t0, nt):
            f = bcol[t - t0] * inv
            b[t] = b[t] - f * uupd
            li[t] = li[t] - f * lirow
        face_ref[k:k + 1, :] = jnp.where(lane >= k, rsig, lrow)[0:1]
        u_ref[k:k + 1, :] = urow[0:1]
        rit_ref[k:k + 1, :] = (-sgn * rirow)[0:1]
        li_ref[k:k + 1, :] = lirow[0:1]
        invs.append(inv)
    tau_ref[...] = tau_row[0:1]
    facet_ref[...] = face_ref[...].T
    umat = u_ref[...]
    ut = umat.T
    u_t = [ut[8 * t:8 * t + 8, :] for t in range(nt)]
    e = [jnp.where(lane == sub + 8 * t, 1.0, 0.0) for t in range(nt)]
    for k in range(NC):
        t0, s = divmod(k, 8)
        yrow = row_of(e[t0], s) * invs[k]
        uit_ref[k:k + 1, :] = yrow[0:1]
        for t in range(t0, nt):
            e[t] = e[t] - col_of(u_t[t], k) * yrow
    limat = li_ref[...]
    nmat_ref[...] = dot_tn(limat, uit_ref[...])
    tful = -dot_nt(dot_nt(umat, rit_ref[...]), limat)
    rows = lax.broadcasted_iota(jnp.int32, (NC, NC), 0)
    cols = lax.broadcasted_iota(jnp.int32, (NC, NC), 1)
    tful = jnp.where(cols > rows, tful, 0.0)
    tful = jnp.where(cols == rows, jnp.broadcast_to(tau_row[0:1], (NC, NC)), tful)
    for j in range(PANELS):
        tfac_ref[j] = tful[j * BW:(j + 1) * BW, j * BW:(j + 1) * BW]


def factor(gram, ptop):
    sq = jax.ShapeDtypeStruct((NC, NC), jnp.float32)
    return pl.pallas_call(
        factor_kernel,
        out_shape=(sq, jax.ShapeDtypeStruct((PANELS, BW, BW), jnp.float32), jax.ShapeDtypeStruct((1, NC), jnp.float32), sq, sq, sq),
        in_specs=[pl.BlockSpec(memory_space=pltpu.VMEM)] * 2,
        out_specs=tuple([pl.BlockSpec(memory_space=pltpu.VMEM)] * 6),
        scratch_shapes=[pltpu.VMEM((NC, NC), jnp.float32)] * 3,
        cost_estimate=pl.CostEstimate(flops=400_000_000, bytes_accessed=600_000, transcendentals=0),
        name="factor",
    )(gram, ptop)


def gather_kernel(at_ref, pt_out, xh_out, g_out, ptop_out, head_out,
                  a_v, pt_v, x_v, g_v, g_in, x_in, head_v, ptop_v,
                  a_sem, own_sem, send_r, send_l, recv, h_sem, hsend, hrecv, psend, precv, gsend, grecv, xsend, xrecv, out_sem):
    ncol, local_rows = at_ref.shape
    nch = local_rows // CH
    half = ncol // 2
    q = lax.axis_index('col')
    r = lax.axis_index('row')
    last = lax.axis_size('col') - 1

    def own_load(c):
        return pltpu.make_async_copy(at_ref.at[pl.ds(0, BW), pl.ds(c * CH, CH)], pt_v.at[c, q], own_sem.at[c])

    def a_load(c):
        return pltpu.make_async_copy(at_ref.at[:, pl.ds(c * CH, CH)], a_v.at[c], a_sem.at[c])

    def pt_store(c):
        return pltpu.make_async_copy(pt_v.at[c], pt_out.at[:, :, pl.ds(c * CH, CH)], out_sem.at[c])

    def hop(c, j, to, sems):
        return pltpu.make_async_remote_copy(
            src_ref=pt_v.at[c, j], dst_ref=pt_v.at[c, j], send_sem=sems.at[c, j], recv_sem=recv.at[c, j],
            device_id={'col': to}, device_id_type=MESH)

    def head_send(p):
        return pltpu.make_async_remote_copy(
            src_ref=at_ref.at[:, pl.ds(0, NC)], dst_ref=head_v, send_sem=hsend.at[p], recv_sem=hrecv,
            device_id={'row': p}, device_id_type=MESH)

    def ptop_send(p):
        return pltpu.make_async_remote_copy(
            src_ref=pt_v.at[0, :, :, pl.ds(0, NC)], dst_ref=ptop_v, send_sem=psend.at[p], recv_sem=precv,
            device_id={'row': p}, device_id_type=MESH)

    for c in range(nch):
        own_load(c).start()
    for c in range(nch):
        a_load(c).start()

    barrier = pltpu.get_barrier_semaphore()

    @pl.when(q > 0)
    def _():
        pl.semaphore_signal(barrier, inc=1, device_id={'col': q - 1}, device_id_type=MESH)

    @pl.when(q < last)
    def _():
        pl.semaphore_signal(barrier, inc=1, device_id={'col': q + 1}, device_id_type=MESH)

    for d in range(1, 4):
        pl.semaphore_signal(barrier, inc=1, device_id={'row': (r + d) % 4}, device_id_type=MESH)
    inner = jnp.logical_and(q > 0, q < last)

    @pl.when(inner)
    def _():
        pl.semaphore_wait(barrier, 5)

    @pl.when(jnp.logical_not(inner))
    def _():
        pl.semaphore_wait(barrier, 4)

    for c in range(nch):
        own_load(c).wait()

        @pl.when(q < last)
        def _():
            hop(c, q, q + 1, send_r).start()

        @pl.when(q > 0)
        def _():
            hop(c, q, q - 1, send_l).start()

    head_local = pltpu.make_async_copy(at_ref.at[:, pl.ds(0, NC)], head_v, h_sem)

    @pl.when(r == 0)
    def _():
        for p in range(1, 4):
            head_send(p).start()
        head_local.start()

    x_v[...] = jnp.zeros_like(x_v)
    g_v[...] = jnp.zeros_like(g_v)

    def chunk(c, carry):
        for d in range(1, 4):
            @pl.when(q >= d)
            def _():
                hop(c, q - d, q, send_r).wait_recv()

                @pl.when(q < last)
                def _():
                    hop(c, q - d, q + 1, send_r).start()

            @pl.when(q + d <= last)
            def _():
                hop(c, q + d, q, send_l).wait_recv()

                @pl.when(q > 0)
                def _():
                    hop(c, q + d, q - 1, send_l).start()

        pt_store(c).start()

        @pl.when(jnp.logical_and(c == 0, r == 0))
        def _():
            for p in range(1, 4):
                ptop_send(p).start()
            for j in range(PANELS):
                ptop_out[j * BW:(j + 1) * BW, :] = pt_v[0, j, :, 0:NC]

        a_load(c).wait()
        p = pt_v[c].reshape(NC, CH)
        x_v[...] += dot_nt(a_v[c], p)
        g_v[...] += dot_nt(p, p)
        return carry

    lax.fori_loop(0, nch, chunk, 0)

    core = r % 2
    mate = r + 1 - 2 * core
    x_copy = pltpu.make_async_remote_copy(
        src_ref=x_v.at[pl.ds(half * (1 - core), half)], dst_ref=x_in, send_sem=xsend, recv_sem=xrecv,
        device_id={'row': mate}, device_id_type=MESH)
    x_copy.start()
    g_copies = []
    for d in range(1, 4):
        g_copies.append(pltpu.make_async_remote_copy(
            src_ref=g_v, dst_ref=g_in.at[d - 1], send_sem=gsend.at[d - 1], recv_sem=grecv.at[d - 1],
            device_id={'row': (r + d) % 4}, device_id_type=MESH))
        g_copies[-1].start()

    @pl.when(r == 0)
    def _():
        for p in range(1, 4):
            head_send(p).wait_send()
            ptop_send(p).wait_send()
        head_local.wait()

    @pl.when(r > 0)
    def _():
        head_send(0).wait_recv()
        ptop_send(0).wait_recv()
        for j in range(PANELS):
            ptop_out[j * BW:(j + 1) * BW, :] = ptop_v[j]

    head_store = pltpu.make_async_copy(head_v, head_out, h_sem)
    head_store.start()

    def drain(c, carry):
        pt_store(c).wait()
        for j in range(PANELS):
            @pl.when(jnp.logical_and(j <= q, q < last))
            def _():
                hop(c, j, q + 1, send_r).wait_send()

            @pl.when(jnp.logical_and(j >= q, q > 0))
            def _():
                hop(c, j, q - 1, send_l).wait_send()
        return carry

    lax.fori_loop(0, nch, drain, 0)
    for g_copy in g_copies:
        g_copy.wait()
    parts = [g_v[...]] + [g_in[d - 1] for d in range(1, 4)]
    total = None
    for row in range(4):
        dist = (r - row + 4) % 4
        part = jnp.where(dist == 0, parts[0], jnp.where(dist == 1, parts[1], jnp.where(dist == 2, parts[2], parts[3])))
        total = part if total is None else total + part
    g_out[...] = total
    x_copy.wait()
    xh_out[...] = x_v[pl.ds(half * core, half), :] + x_in[...]
    head_store.wait()


def gather(at):
    ncol, local_rows = at.shape
    nch = local_rows // CH
    f32 = jnp.float32
    vm, anys = pl.BlockSpec(memory_space=pltpu.VMEM), pl.BlockSpec(memory_space=pl.ANY)
    dma = pltpu.SemaphoreType.DMA
    return pl.pallas_call(
        gather_kernel,
        out_shape=(jax.ShapeDtypeStruct((PANELS, BW, local_rows), f32), jax.ShapeDtypeStruct((ncol // 2, NC), f32),
                   jax.ShapeDtypeStruct((NC, NC), f32), jax.ShapeDtypeStruct((NC, NC), f32), jax.ShapeDtypeStruct((ncol, NC), f32)),
        in_specs=[anys],
        out_specs=(anys, vm, vm, vm, anys),
        scratch_shapes=[pltpu.VMEM((nch, ncol, CH), f32), pltpu.VMEM((nch, PANELS, BW, CH), f32), pltpu.VMEM((ncol, NC), f32),
                        pltpu.VMEM((NC, NC), f32), pltpu.VMEM((3, NC, NC), f32), pltpu.VMEM((ncol // 2, NC), f32),
                        pltpu.VMEM((ncol, NC), f32), pltpu.VMEM((PANELS, BW, NC), f32),
                        dma((nch,)), dma((nch,)), dma((nch, 4)), dma((nch, 4)), dma((nch, 4)), dma, dma((4,)), dma, dma((4,)), dma,
                        dma((3,)), dma((3,)), dma, dma, dma((nch,))],
        compiler_params=pltpu.CompilerParams(collective_id=0, has_side_effects=True, vmem_limit_bytes=48 * 1024 * 1024),
        name="gather",
    )(at)


def split3(x):
    hi = x.astype(jnp.bfloat16)
    rem = x - hi.astype(jnp.float32)
    mid = rem.astype(jnp.bfloat16)
    lo = (rem - mid.astype(jnp.float32)).astype(jnp.bfloat16)
    return hi, mid, lo


def update_kernel(at_ref, pt_ref, x0_ref, x1_ref, x2_ref, x3_ref, head_ref, rit_ref, nmat_ref, uit_ref, facet_ref, out_ref, zhm_v, zhl_v, top_v):
    step = pl.program_id(0)
    q = lax.axis_index('col')
    r = lax.axis_index('row')
    ncol = head_ref.shape[0]
    half = ncol // 2

    @pl.when(step == 0)
    def _():
        core = r % 2
        rit = rit_ref[...]
        nmat = nmat_ref[...]
        mine = pl.multiple_of(half * core, half)
        other = pl.multiple_of(half * (1 - core), half)
        for lo, xa, xb in ((mine, x0_ref, x1_ref), (other, x2_ref, x3_ref)):
            r12t = dot_nt(xa[...] + xb[...], rit)
            top_v[pl.ds(lo, half), :] = r12t
            z = dot_nn(head_ref[pl.ds(lo, half), :] - r12t, nmat)
            zh, zm, zl = split3(z)
            zhm_v[pl.ds(lo, half), 0:NC] = zh
            zhm_v[pl.ds(lo, half), NC:2 * NC] = zm
            zhl_v[pl.ds(lo, half), 0:NC] = zh
            zhl_v[pl.ds(lo, half), NC:2 * NC] = zl
        own = pl.ds(pl.multiple_of(q * BW, BW), BW)
        top_v[0:BW, :] = facet_ref[own, :]
        zh, zm, zl = split3(-uit_ref[own, :])
        zhm_v[0:BW, 0:NC] = zh
        zhm_v[0:BW, NC:2 * NC] = zm
        zhl_v[0:BW, 0:NC] = zh
        zhl_v[0:BW, NC:2 * NC] = zl

    ph, pm, plo = split3(pt_ref[...].reshape(NC, pt_ref.shape[2]))
    w_hm = jnp.concatenate([ph, pm], axis=0)
    w_mh = jnp.concatenate([pm, ph], axis=0)
    w_lh = jnp.concatenate([plo, ph], axis=0)

    def dot16(x, y):
        return lax.dot_general(x, y, (((1,), (0,)), ((), ())), preferred_element_type=jnp.float32)

    zhm = zhm_v[...]
    prod = dot16(zhm, w_hm) + (dot16(zhm, w_mh) + dot16(zhl_v[...], w_lh))
    out_ref[BW:, :] = at_ref[BW:, :] - prod[BW:]
    out_ref[0:BW, :] = -prod[0:BW]

    @pl.when(jnp.logical_and(step == 0, r == 0))
    def _():
        out_ref[:, 0:NC] = top_v[...]


def update(at, pt, xs, head, rit, nmat, uit, facet):
    ncol, local_rows = at.shape
    lanes = 512
    full = lambda a: pl.BlockSpec(a.shape, lambda i: (0,) * a.ndim)
    strip = pl.BlockSpec((ncol, lanes), lambda i: (0, i))
    return pl.pallas_call(
        update_kernel,
        grid=(local_rows // lanes,),
        out_shape=jax.ShapeDtypeStruct(at.shape, jnp.float32),
        in_specs=[strip, pl.BlockSpec((PANELS, BW, lanes), lambda i: (0, 0, i))] + [full(x) for x in xs]
        + [full(head), full(rit), full(nmat), full(uit), full(facet)],
        out_specs=strip,
        scratch_shapes=[pltpu.VMEM((ncol, 2 * NC), jnp.bfloat16), pltpu.VMEM((ncol, 2 * NC), jnp.bfloat16), pltpu.VMEM((ncol, NC), jnp.float32)],
        compiler_params=pltpu.CompilerParams(dimension_semantics=("arbitrary",), vmem_limit_bytes=48 * 1024 * 1024),
        name="update",
    )(at, pt, *xs, head, rit, nmat, uit, facet)


def solution(mesh):
    block_spec = P(('batch', 'row'), 'col', None)

    def device_fn(a_local):
        local_rows, local_blocks, bw = a_local.shape
        ncol = local_blocks * bw
        at = a_local.transpose(1, 2, 0).reshape(ncol, local_rows)
        pt, xh, gram, ptop, head = gather(at)
        x1, x2, x3 = [lax.ppermute(xh, 'row', [(i, i ^ b) for i in range(4)]) for b in (2, 1, 3)]
        facet, tfac, tau, rit, nmat, uit = factor(gram, ptop)
        out = update(at, pt, (xh, x1, x2, x3), head, rit, nmat, uit, facet)
        a_out = out.reshape(local_blocks, bw, local_rows).transpose(2, 0, 1)
        return a_out, tau.reshape(NC), tfac

    return jax.shard_map(device_fn, mesh=mesh, in_specs=(block_spec,), out_specs=(block_spec, P('batch'), P('batch', None, None)), check_vma=False)
```

```python
import functools
import jax
import jax.numpy as jnp
from jax import lax
from jax.experimental import pallas as pl
from jax.experimental.pallas import tpu as pltpu
from jax.sharding import PartitionSpec as P

PANELS = 4
BW = 32
NC = PANELS * BW
CH = 512
UPDATE_VMEM = 32 * 1024 * 1024
GATHER_VMEM = 32 * 1024 * 1024
AHEAD = 3
HIGHEST = lax.Precision.HIGHEST
MESH = pl.DeviceIdType.MESH


def dot_nn(x, y):
    return lax.dot_general(x, y, (((1,), (0,)), ((), ())), precision=HIGHEST, preferred_element_type=jnp.float32)


def dot_nt(x, y):
    return lax.dot_general(x, y, (((1,), (1,)), ((), ())), precision=HIGHEST, preferred_element_type=jnp.float32)


def dot_tn(x, y):
    return lax.dot_general(x, y, (((0,), (0,)), ((), ())), precision=HIGHEST, preferred_element_type=jnp.float32)


def factor_kernel(g_ref, ptop_ref, facet_ref, tfac_ref, tau_ref, rit_ref, nmat_ref, uit_ref, u_ref, li_ref, face_ref):
    nt = NC // 8
    lane = lax.broadcasted_iota(jnp.int32, (8, NC), 1)
    sub = lax.broadcasted_iota(jnp.int32, (8, NC), 0)

    def row_of(tile, s):
        return jnp.broadcast_to(tile[s:s + 1, :], (8, NC))

    def col_of(tile, k):
        return jnp.broadcast_to(tile[:, k:k + 1], (8, NC))

    g = [g_ref[8 * t:8 * t + 8, :] for t in range(nt)]
    top = ptop_ref[...].T
    b = [top[8 * t:8 * t + 8, :] for t in range(nt)]
    ri = [jnp.where(lane == sub + 8 * t, 1.0, 0.0) for t in range(nt)]
    li = [jnp.where(lane == sub + 8 * t, 1.0, 0.0) for t in range(nt)]
    inv_row = jnp.zeros((8, NC), jnp.float32)
    tau_row = jnp.zeros((8, NC), jnp.float32)
    invs = []
    for k in range(NC):
        t0, s = divmod(k, 8)
        gcol = [col_of(g[t], k) for t in range(t0, nt)]
        bcol = [col_of(b[t], k) for t in range(t0, nt)]
        diag = row_of(gcol[0], s)
        rs = lax.rsqrt(diag)
        rrow = jnp.where(lane >= k, row_of(g[t0], s) * rs, 0.0)
        rirow = row_of(ri[t0], s) * rs
        for t in range(t0, nt):
            f = gcol[t - t0] * rs
            g[t] = g[t] - f * rrow
            ri[t] = ri[t] - f * rirow
        norm = diag * rs
        alpha = row_of(bcol[0], s)
        sgn = jnp.where(alpha >= 0.0, 1.0, -1.0)
        beta = -sgn * norm
        rsig = -sgn * rrow
        brow = row_of(b[t0], s)
        urow = jnp.where(lane >= k, brow - rsig, 0.0)
        piv = alpha - beta
        inv = 1.0 / piv
        tau_row = jnp.where(lane == k, (beta - alpha) / beta, tau_row)
        lrow = brow * inv_row
        inv_row = jnp.where(lane == k, inv, inv_row)
        uupd = jnp.where(lane > k, urow, 0.0)
        lirow = row_of(li[t0], s)
        for t in range(t0, nt):
            f = bcol[t - t0] * inv
            b[t] = b[t] - f * uupd
            li[t] = li[t] - f * lirow
        face_ref[k:k + 1, :] = jnp.where(lane >= k, rsig, lrow)[0:1]
        u_ref[k:k + 1, :] = urow[0:1]
        rit_ref[k:k + 1, :] = (-sgn * rirow)[0:1]
        li_ref[k:k + 1, :] = lirow[0:1]
        invs.append(inv)
    tau_ref[...] = tau_row[0:1]
    facet_ref[...] = face_ref[...].T
    umat = u_ref[...]
    ut = umat.T
    u_t = [ut[8 * t:8 * t + 8, :] for t in range(nt)]
    e = [jnp.where(lane == sub + 8 * t, 1.0, 0.0) for t in range(nt)]
    for k in range(NC):
        t0, s = divmod(k, 8)
        yrow = row_of(e[t0], s) * invs[k]
        uit_ref[k:k + 1, :] = yrow[0:1]
        for t in range(t0, nt):
            e[t] = e[t] - col_of(u_t[t], k) * yrow
    limat = li_ref[...]
    nmat_ref[...] = dot_tn(limat, uit_ref[...])
    tful = -dot_nt(dot_nt(umat, rit_ref[...]), limat)
    rows = lax.broadcasted_iota(jnp.int32, (NC, NC), 0)
    cols = lax.broadcasted_iota(jnp.int32, (NC, NC), 1)
    tful = jnp.where(cols > rows, tful, 0.0)
    tful = jnp.where(cols == rows, jnp.broadcast_to(tau_row[0:1], (NC, NC)), tful)
    for j in range(PANELS):
        tfac_ref[j] = tful[j * BW:(j + 1) * BW, j * BW:(j + 1) * BW]


def factor(gram, ptop):
    sq = jax.ShapeDtypeStruct((NC, NC), jnp.float32)
    return pl.pallas_call(
        factor_kernel,
        out_shape=(sq, jax.ShapeDtypeStruct((PANELS, BW, BW), jnp.float32), jax.ShapeDtypeStruct((1, NC), jnp.float32), sq, sq, sq),
        in_specs=[pl.BlockSpec(memory_space=pltpu.VMEM)] * 2,
        out_specs=tuple([pl.BlockSpec(memory_space=pltpu.VMEM)] * 6),
        scratch_shapes=[pltpu.VMEM((NC, NC), jnp.float32)] * 3,
        compiler_params=pltpu.CompilerParams(vmem_limit_bytes=8 * 1024 * 1024),
        cost_estimate=pl.CostEstimate(flops=400_000_000, bytes_accessed=600_000, transcendentals=0),
        name="factor",
    )(gram, ptop)


def gather_kernel(at_ref, a_v, pt_out, xh_out, g_out, ptop_out, head_out,
                  pt_v, x_v, g_v, g_in, x_in, head_v, ptop_v,
                  a_sem, own_sem, send, fwd, recv, h_sem, hsend, hrecv, psend, precv, gsend, grecv, xsend, xrecv):
    ncol, local_rows = at_ref.shape
    nch = local_rows // CH
    half = ncol // 2
    q = lax.axis_index('col')
    r = lax.axis_index('row')
    last = lax.axis_size('col') - 1

    def own_load(c):
        return pltpu.make_async_copy(at_ref.at[pl.ds(0, BW), pl.ds(c * CH, CH)], pt_v.at[c, q], own_sem.at[c])

    def a_load(c):
        return pltpu.make_async_copy(at_ref.at[:, pl.ds(c * CH, CH)], a_v.at[c], a_sem.at[c])

    def hop(c, j, to, sem):
        return pltpu.make_async_remote_copy(
            src_ref=pt_v.at[c, j], dst_ref=pt_v.at[c, j], send_sem=sem, recv_sem=recv.at[c, j],
            device_id={'col': to}, device_id_type=MESH)

    routes = ((q + 2, q + 2 <= last, 0), (q - 2, q >= 2, 1), (q + 1, q < last, 2), (q - 1, q > 0, 3))

    def send_own(c):
        own_load(c).wait()
        for to, valid, slot in routes:
            @pl.when(valid)
            def _():
                hop(c, q, to, send.at[c, slot]).start()

    def head_send(p):
        return pltpu.make_async_remote_copy(
            src_ref=at_ref.at[:, pl.ds(0, NC)], dst_ref=head_v, send_sem=hsend.at[p], recv_sem=hrecv,
            device_id={'row': p}, device_id_type=MESH)

    def ptop_send(p):
        return pltpu.make_async_remote_copy(
            src_ref=pt_v.at[0, :, :, pl.ds(0, NC)], dst_ref=ptop_v, send_sem=psend.at[p], recv_sem=precv,
            device_id={'row': p}, device_id_type=MESH)

    for c in range(nch):
        own_load(c).start()
    for c in range(nch):
        a_load(c).start()

    barrier = pltpu.get_barrier_semaphore()

    for to, valid, _ in routes:
        @pl.when(valid)
        def _():
            pl.semaphore_signal(barrier, inc=1, device_id={'col': to}, device_id_type=MESH)

    for d in range(1, 4):
        pl.semaphore_signal(barrier, inc=1, device_id={'row': (r + d) % 4}, device_id_type=MESH)
    inner = jnp.logical_and(q > 0, q < last)

    @pl.when(inner)
    def _():
        pl.semaphore_wait(barrier, 6)

    @pl.when(jnp.logical_not(inner))
    def _():
        pl.semaphore_wait(barrier, 5)

    for c in range(min(AHEAD, nch)):
        send_own(c)

    head_local = pltpu.make_async_copy(at_ref.at[:, pl.ds(0, NC)], head_v, h_sem)

    @pl.when(r == 0)
    def _():
        for p in range(1, 4):
            head_send(p).start()
        head_local.start()

    x_v[...] = jnp.zeros_like(x_v)
    g_v[...] = jnp.zeros_like(g_v)

    def chunk(c, carry):
        @pl.when(c + AHEAD < nch)
        def _():
            send_own(c + AHEAD)

        for d in range(1, 4):
            @pl.when(q >= d)
            def _():
                hop(c, q - d, q, fwd.at[c]).wait_recv()

            @pl.when(q + d <= last)
            def _():
                hop(c, q + d, q, fwd.at[c]).wait_recv()

            if d == 2:
                @pl.when(q == last - 1)
                def _():
                    hop(c, 0, q + 1, fwd.at[c]).start()

                @pl.when(q == 1)
                def _():
                    hop(c, last, q - 1, fwd.at[c]).start()

        pt_out[c] = pt_v[c]

        @pl.when(jnp.logical_and(c == 0, r == 0))
        def _():
            for p in range(1, 4):
                ptop_send(p).start()
            for j in range(PANELS):
                ptop_out[j * BW:(j + 1) * BW, :] = pt_v[0, j, :, 0:NC]

        a_load(c).wait()
        p = pt_v[c].reshape(NC, CH)
        x_v[...] += dot_nt(a_v[c], p)
        g_v[...] += dot_nt(p, p)
        return carry

    lax.fori_loop(0, nch, chunk, 0)

    core = r % 2
    mate = r + 1 - 2 * core
    x_copy = pltpu.make_async_remote_copy(
        src_ref=x_v.at[pl.ds(half * (1 - core), half)], dst_ref=x_in, send_sem=xsend, recv_sem=xrecv,
        device_id={'row': mate}, device_id_type=MESH)
    x_copy.start()
    g_copies = []
    for d in range(1, 4):
        g_copies.append(pltpu.make_async_remote_copy(
            src_ref=g_v, dst_ref=g_in.at[d - 1], send_sem=gsend.at[d - 1], recv_sem=grecv.at[d - 1],
            device_id={'row': (r + d) % 4}, device_id_type=MESH))
        g_copies[-1].start()

    @pl.when(r == 0)
    def _():
        for p in range(1, 4):
            head_send(p).wait_send()
            ptop_send(p).wait_send()
        head_local.wait()

    @pl.when(r > 0)
    def _():
        head_send(0).wait_recv()
        ptop_send(0).wait_recv()
        for j in range(PANELS):
            ptop_out[j * BW:(j + 1) * BW, :] = ptop_v[j]

    head_out[...] = head_v[...]

    def drain(c, carry):
        for to, valid, slot in routes:
            @pl.when(valid)
            def _():
                hop(c, q, to, send.at[c, slot]).wait_send()

        @pl.when(inner)
        def _():
            hop(c, q, q, fwd.at[c]).wait_send()

        return carry

    lax.fori_loop(0, nch, drain, 0)
    for g_copy in g_copies:
        g_copy.wait()
    parts = [g_v[...]] + [g_in[d - 1] for d in range(1, 4)]
    total = None
    for row in range(4):
        dist = (r - row + 4) % 4
        part = jnp.where(dist == 0, parts[0], jnp.where(dist == 1, parts[1], jnp.where(dist == 2, parts[2], parts[3])))
        total = part if total is None else total + part
    g_out[...] = total
    x_copy.wait()
    xh_out[...] = x_v[pl.ds(half * core, half), :] + x_in[...]


def gather(at):
    ncol, local_rows = at.shape
    nch = local_rows // CH
    f32 = jnp.float32
    vm, anys = pl.BlockSpec(memory_space=pltpu.VMEM), pl.BlockSpec(memory_space=pl.ANY)
    dma = pltpu.SemaphoreType.DMA
    return pl.pallas_call(
        gather_kernel,
        out_shape=(jax.ShapeDtypeStruct((nch, ncol, CH), f32), jax.ShapeDtypeStruct((nch, PANELS, BW, CH), f32), jax.ShapeDtypeStruct((ncol // 2, NC), f32),
                   jax.ShapeDtypeStruct((NC, NC), f32), jax.ShapeDtypeStruct((NC, NC), f32), jax.ShapeDtypeStruct((ncol, NC), f32)),
        in_specs=[anys],
        out_specs=(vm,) * 6,
        scratch_shapes=[pltpu.VMEM((nch, PANELS, BW, CH), f32), pltpu.VMEM((ncol, NC), f32),
                        pltpu.VMEM((NC, NC), f32), pltpu.VMEM((3, NC, NC), f32), pltpu.VMEM((ncol // 2, NC), f32),
                        pltpu.VMEM((ncol, NC), f32), pltpu.VMEM((PANELS, BW, NC), f32),
                        dma((nch,)), dma((nch,)), dma((nch, 4)), dma((nch,)), dma((nch, 4)), dma, dma((4,)), dma, dma((4,)), dma,
                        dma((3,)), dma((3,)), dma, dma],
        compiler_params=pltpu.CompilerParams(collective_id=0, has_side_effects=True, vmem_limit_bytes=GATHER_VMEM),
        name="gather",
    )(at)


def split3(x):
    hi = x.astype(jnp.bfloat16)
    rem = x - hi.astype(jnp.float32)
    mid = rem.astype(jnp.bfloat16)
    lo = (rem - mid.astype(jnp.float32)).astype(jnp.bfloat16)
    return hi, mid, lo


def store_split(dst, rows, z):
    zh, zm, zl = split3(z)
    for i, part in enumerate((zh, zm, zh, zm, zh, zl)):
        dst[rows, i * NC:(i + 1) * NC] = part


def update_kernel(a_ref, pt_ref, x0_ref, x1_ref, x2_ref, x3_ref, head_ref, rit_ref, nmat_ref, uit_ref, facet_ref, out_ref, z_v, top_v):
    step = pl.program_id(0)
    q = lax.axis_index('col')
    r = lax.axis_index('row')
    ncol = head_ref.shape[0]
    half = ncol // 2

    @pl.when(step == 0)
    def _():
        core = r % 2
        rit = rit_ref[...]
        nmat = nmat_ref[...]
        mine = pl.multiple_of(half * core, half)
        other = pl.multiple_of(half * (1 - core), half)
        for lo, xa, xb in ((mine, x0_ref, x1_ref), (other, x2_ref, x3_ref)):
            r12t = dot_nt(xa[...] + xb[...], rit)
            top_v[pl.ds(lo, half), :] = r12t
            store_split(z_v, pl.ds(lo, half), dot_nn(head_ref[pl.ds(lo, half), :] - r12t, nmat))
        own = pl.ds(pl.multiple_of(q * BW, BW), BW)
        top_v[0:BW, :] = facet_ref[own, :]
        store_split(z_v, pl.ds(0, BW), -uit_ref[own, :])

    ph, pm, plo = split3(pt_ref[step].reshape(NC, CH))
    wide = jnp.concatenate([ph, pm, pm, ph, plo, ph], axis=0)
    prod = lax.dot_general(z_v[...], wide, (((1,), (0,)), ((), ())), preferred_element_type=jnp.float32)
    out_ref[BW:, :] = a_ref[step, BW:, :] - prod[BW:]
    out_ref[0:BW, :] = -prod[0:BW]

    @pl.when(jnp.logical_and(step == 0, r == 0))
    def _():
        out_ref[:, 0:NC] = top_v[...]


def update(a, pt, xs, head, rit, nmat, uit, facet):
    nch, ncol, _ = a.shape
    vm = pl.BlockSpec(memory_space=pltpu.VMEM)
    return pl.pallas_call(
        update_kernel,
        grid=(nch,),
        out_shape=jax.ShapeDtypeStruct((ncol, nch * CH), jnp.float32),
        in_specs=[vm] * 11,
        out_specs=pl.BlockSpec((ncol, CH), lambda i: (0, i)),
        scratch_shapes=[pltpu.VMEM((ncol, 6 * NC), jnp.bfloat16), pltpu.VMEM((ncol, NC), jnp.float32)],
        compiler_params=pltpu.CompilerParams(dimension_semantics=("arbitrary",), vmem_limit_bytes=UPDATE_VMEM),
        name="update",
    )(a, pt, *xs, head, rit, nmat, uit, facet)


def solution(mesh):
    block_spec = P(('batch', 'row'), 'col', None)

    def device_fn(a_local):
        local_rows, local_blocks, bw = a_local.shape
        ncol = local_blocks * bw
        at = a_local.transpose(1, 2, 0).reshape(ncol, local_rows)
        a, pt, xh, gram, ptop, head = gather(at)
        x1, x2, x3 = [lax.ppermute(xh, 'row', [(i, i ^ b) for i in range(4)]) for b in (2, 1, 3)]
        facet, tfac, tau, rit, nmat, uit = factor(gram, ptop)
        out = update(a, pt, (xh, x1, x2, x3), head, rit, nmat, uit, facet)
        a_out = out.reshape(local_blocks, bw, local_rows).transpose(2, 0, 1)
        return a_out, tau.reshape(NC), tfac

    return jax.shard_map(device_fn, mesh=mesh, in_specs=(block_spec,), out_specs=(block_spec, P('batch'), P('batch', None, None)), check_vma=False)
```

```python
import functools
import jax
import jax.numpy as jnp
from jax import lax
from jax.experimental import pallas as pl
from jax.experimental.pallas import tpu as pltpu
from jax.sharding import PartitionSpec as P

PANELS = 4
BW = 32
NC = PANELS * BW
CH = 512
UPDATE_VMEM = 32 * 1024 * 1024
GATHER_VMEM = 32 * 1024 * 1024
AHEAD = 3
HIGHEST = lax.Precision.HIGHEST
MESH = pl.DeviceIdType.MESH


def dot_nn(x, y):
    return lax.dot_general(x, y, (((1,), (0,)), ((), ())), precision=HIGHEST, preferred_element_type=jnp.float32)


def dot_nt(x, y):
    return lax.dot_general(x, y, (((1,), (1,)), ((), ())), precision=HIGHEST, preferred_element_type=jnp.float32)


def dot_tn(x, y):
    return lax.dot_general(x, y, (((0,), (0,)), ((), ())), precision=HIGHEST, preferred_element_type=jnp.float32)


def factor_kernel(g_ref, ptop_ref, facet_ref, tfac_ref, tau_ref, rit_ref, nmat_ref, uit_ref, u_ref, li_ref, face_ref):
    nt = NC // 8
    lane = lax.broadcasted_iota(jnp.int32, (8, NC), 1)
    sub = lax.broadcasted_iota(jnp.int32, (8, NC), 0)

    def row_of(tile, s):
        return jnp.broadcast_to(tile[s:s + 1, :], (8, NC))

    def col_of(tile, k):
        return jnp.broadcast_to(tile[:, k:k + 1], (8, NC))

    g = [g_ref[8 * t:8 * t + 8, :] for t in range(nt)]
    top = ptop_ref[...].T
    b = [top[8 * t:8 * t + 8, :] for t in range(nt)]
    ri = [jnp.where(lane == sub + 8 * t, 1.0, 0.0) for t in range(nt)]
    li = [jnp.where(lane == sub + 8 * t, 1.0, 0.0) for t in range(nt)]
    inv_row = jnp.zeros((8, NC), jnp.float32)
    tau_row = jnp.zeros((8, NC), jnp.float32)
    invs = []

    def trail(t, block, steps, width):
        for lo in range(0, 8, width):
            cg = {s: col_of(g[t], 8 * block + s) for s in range(lo, lo + width)}
            cb = {s: col_of(b[t], 8 * block + s) for s in range(lo, lo + width)}
            for s in range(lo, lo + width):
                rs, inv, rrow, rirow, uupd, lirow, rj, uj = steps[s]
                fg = cg[s] * rs
                fb = cb[s] * inv
                g[t] = g[t] - fg * rrow
                ri[t] = ri[t] - fg * rirow
                b[t] = b[t] - fb * uupd
                li[t] = li[t] - fb * lirow
                for j in range(s + 1, lo + width):
                    cg[j] = cg[j] - fg * rj[j]
                    cb[j] = cb[j] - fb * uj[j]

    pending = []
    for block in range(nt):
        gd, bd, rid, lid = g[block], b[block], ri[block], li[block]
        cg = [col_of(gd, 8 * block + s) for s in range(8)]
        cb = [col_of(bd, 8 * block + s) for s in range(8)]
        steps = []
        share = -(-len(pending) // 8)
        for s in range(8):
            k = 8 * block + s
            diag = row_of(cg[s], s)
            rs = lax.rsqrt(diag)
            norm = diag * rs
            alpha = row_of(cb[s], s)
            sgn = jnp.where(alpha >= 0.0, 1.0, -1.0)
            beta = -sgn * norm
            inv = 1.0 / (alpha - beta)
            fg = cg[s] * rs
            fb = cb[s] * inv
            rj, uj = {}, {}
            for j in range(s + 1, 8):
                rj[j] = row_of(fg, j)
                uj[j] = row_of(cb[j], s) + sgn * rj[j]
                cg[j] = cg[j] - fg * rj[j]
                cb[j] = cb[j] - fb * uj[j]
            rrow = jnp.where(lane >= k, row_of(gd, s) * rs, 0.0)
            rirow = row_of(rid, s) * rs
            lirow = row_of(lid, s)
            brow = row_of(bd, s)
            rsig = -sgn * rrow
            urow = jnp.where(lane >= k, brow - rsig, 0.0)
            uupd = jnp.where(lane > k, urow, 0.0)
            gd = gd - fg * rrow
            rid = rid - fg * rirow
            bd = bd - fb * uupd
            lid = lid - fb * lirow
            steps.append((rs, inv, rrow, rirow, uupd, lirow, rj, uj))
            tau_row = jnp.where(lane == k, (beta - alpha) / beta, tau_row)
            lrow = brow * inv_row
            inv_row = jnp.where(lane == k, inv, inv_row)
            face_ref[k:k + 1, :] = jnp.where(lane >= k, rsig, lrow)[0:1]
            u_ref[k:k + 1, :] = urow[0:1]
            rit_ref[k:k + 1, :] = (-sgn * rirow)[0:1]
            li_ref[k:k + 1, :] = lirow[0:1]
            invs.append(inv)
            for args in pending[:share]:
                trail(*args)
            pending = pending[share:]
        if block + 1 < nt:
            trail(block + 1, block, steps, 8)
        pending = [(t, block, steps, 4) for t in range(block + 2, nt)]
    tau_ref[...] = tau_row[0:1]
    facet_ref[...] = face_ref[...].T
    umat = u_ref[...]
    ut = umat.T
    u_t = [ut[8 * t:8 * t + 8, :] for t in range(nt)]
    e = [jnp.where(lane == sub + 8 * t, 1.0, 0.0) for t in range(nt)]
    for k in range(NC):
        t0, s = divmod(k, 8)
        yrow = row_of(e[t0], s) * invs[k]
        uit_ref[k:k + 1, :] = yrow[0:1]
        for t in range(t0, nt):
            e[t] = e[t] - col_of(u_t[t], k) * yrow
    limat = li_ref[...]
    nmat_ref[...] = dot_tn(limat, uit_ref[...])
    tful = -dot_nt(dot_nt(umat, rit_ref[...]), limat)
    rows = lax.broadcasted_iota(jnp.int32, (NC, NC), 0)
    cols = lax.broadcasted_iota(jnp.int32, (NC, NC), 1)
    tful = jnp.where(cols > rows, tful, 0.0)
    tful = jnp.where(cols == rows, jnp.broadcast_to(tau_row[0:1], (NC, NC)), tful)
    for j in range(PANELS):
        tfac_ref[j] = tful[j * BW:(j + 1) * BW, j * BW:(j + 1) * BW]


def factor(gram, ptop):
    sq = jax.ShapeDtypeStruct((NC, NC), jnp.float32)
    return pl.pallas_call(
        factor_kernel,
        out_shape=(sq, jax.ShapeDtypeStruct((PANELS, BW, BW), jnp.float32), jax.ShapeDtypeStruct((1, NC), jnp.float32), sq, sq, sq),
        in_specs=[pl.BlockSpec(memory_space=pltpu.VMEM)] * 2,
        out_specs=tuple([pl.BlockSpec(memory_space=pltpu.VMEM)] * 6),
        scratch_shapes=[pltpu.VMEM((NC, NC), jnp.float32)] * 3,
        compiler_params=pltpu.CompilerParams(vmem_limit_bytes=8 * 1024 * 1024),
        cost_estimate=pl.CostEstimate(flops=400_000_000, bytes_accessed=600_000, transcendentals=0),
        name="factor",
    )(gram, ptop)


def gather_kernel(at_ref, a_v, pt_out, xh_out, g_out, ptop_out, head_out,
                  pt_v, x_v, g_v, g_in, x_in, head_v, ptop_v,
                  a_sem, own_sem, send, fwd, recv, h_sem, hsend, hrecv, psend, precv, gsend, grecv, xsend, xrecv):
    ncol, local_rows = at_ref.shape
    nch = local_rows // CH
    half = ncol // 2
    q = lax.axis_index('col')
    r = lax.axis_index('row')
    last = lax.axis_size('col') - 1

    def own_load(c):
        return pltpu.make_async_copy(at_ref.at[pl.ds(0, BW), pl.ds(c * CH, CH)], pt_v.at[c, q], own_sem.at[c])

    def a_load(c):
        return pltpu.make_async_copy(at_ref.at[:, pl.ds(c * CH, CH)], a_v.at[c], a_sem.at[c])

    def hop(c, j, to, sem):
        return pltpu.make_async_remote_copy(
            src_ref=pt_v.at[c, j], dst_ref=pt_v.at[c, j], send_sem=sem, recv_sem=recv.at[c, j],
            device_id={'col': to}, device_id_type=MESH)

    routes = ((q + 2, q + 2 <= last, 0), (q - 2, q >= 2, 1), (q + 1, q < last, 2), (q - 1, q > 0, 3))

    def send_own(c):
        own_load(c).wait()
        for to, valid, slot in routes:
            @pl.when(valid)
            def _():
                hop(c, q, to, send.at[c, slot]).start()

    def head_send(p):
        return pltpu.make_async_remote_copy(
            src_ref=at_ref.at[:, pl.ds(0, NC)], dst_ref=head_v, send_sem=hsend.at[p], recv_sem=hrecv,
            device_id={'row': p}, device_id_type=MESH)

    def ptop_send(p):
        return pltpu.make_async_remote_copy(
            src_ref=pt_v.at[0, :, :, pl.ds(0, NC)], dst_ref=ptop_v, send_sem=psend.at[p], recv_sem=precv,
            device_id={'row': p}, device_id_type=MESH)

    for c in range(nch):
        own_load(c).start()
    for c in range(nch):
        a_load(c).start()

    barrier = pltpu.get_barrier_semaphore()

    for to, valid, _ in routes:
        @pl.when(valid)
        def _():
            pl.semaphore_signal(barrier, inc=1, device_id={'col': to}, device_id_type=MESH)

    for d in range(1, 4):
        pl.semaphore_signal(barrier, inc=1, device_id={'row': (r + d) % 4}, device_id_type=MESH)
    inner = jnp.logical_and(q > 0, q < last)

    @pl.when(inner)
    def _():
        pl.semaphore_wait(barrier, 6)

    @pl.when(jnp.logical_not(inner))
    def _():
        pl.semaphore_wait(barrier, 5)

    for c in range(min(AHEAD, nch)):
        send_own(c)

    head_local = pltpu.make_async_copy(at_ref.at[:, pl.ds(0, NC)], head_v, h_sem)

    @pl.when(r == 0)
    def _():
        for p in range(1, 4):
            head_send(p).start()
        head_local.start()

    x_v[...] = jnp.zeros_like(x_v)
    g_v[...] = jnp.zeros_like(g_v)

    def chunk(c, carry):
        @pl.when(c + AHEAD < nch)
        def _():
            send_own(c + AHEAD)

        for d in range(1, 4):
            @pl.when(q >= d)
            def _():
                hop(c, q - d, q, fwd.at[c]).wait_recv()

            @pl.when(q + d <= last)
            def _():
                hop(c, q + d, q, fwd.at[c]).wait_recv()

            if d == 2:
                @pl.when(q == last - 1)
                def _():
                    hop(c, 0, q + 1, fwd.at[c]).start()

                @pl.when(q == 1)
                def _():
                    hop(c, last, q - 1, fwd.at[c]).start()

        pt_out[c] = pt_v[c]

        @pl.when(jnp.logical_and(c == 0, r == 0))
        def _():
            for p in range(1, 4):
                ptop_send(p).start()
            for j in range(PANELS):
                ptop_out[j * BW:(j + 1) * BW, :] = pt_v[0, j, :, 0:NC]

        a_load(c).wait()
        p = pt_v[c].reshape(NC, CH)
        x_v[...] += dot_nt(a_v[c], p)
        g_v[...] += dot_nt(p, p)
        return carry

    lax.fori_loop(0, nch, chunk, 0)

    core = r % 2
    mate = r + 1 - 2 * core
    x_copy = pltpu.make_async_remote_copy(
        src_ref=x_v.at[pl.ds(half * (1 - core), half)], dst_ref=x_in, send_sem=xsend, recv_sem=xrecv,
        device_id={'row': mate}, device_id_type=MESH)
    x_copy.start()
    g_copies = []
    for d in range(1, 4):
        g_copies.append(pltpu.make_async_remote_copy(
            src_ref=g_v, dst_ref=g_in.at[d - 1], send_sem=gsend.at[d - 1], recv_sem=grecv.at[d - 1],
            device_id={'row': (r + d) % 4}, device_id_type=MESH))
        g_copies[-1].start()

    @pl.when(r == 0)
    def _():
        for p in range(1, 4):
            head_send(p).wait_send()
            ptop_send(p).wait_send()
        head_local.wait()

    @pl.when(r > 0)
    def _():
        head_send(0).wait_recv()
        ptop_send(0).wait_recv()
        for j in range(PANELS):
            ptop_out[j * BW:(j + 1) * BW, :] = ptop_v[j]

    head_out[...] = head_v[...]

    def drain(c, carry):
        for to, valid, slot in routes:
            @pl.when(valid)
            def _():
                hop(c, q, to, send.at[c, slot]).wait_send()

        @pl.when(inner)
        def _():
            hop(c, q, q, fwd.at[c]).wait_send()

        return carry

    lax.fori_loop(0, nch, drain, 0)
    for g_copy in g_copies:
        g_copy.wait()
    parts = [g_v[...]] + [g_in[d - 1] for d in range(1, 4)]
    total = None
    for row in range(4):
        dist = (r - row + 4) % 4
        part = jnp.where(dist == 0, parts[0], jnp.where(dist == 1, parts[1], jnp.where(dist == 2, parts[2], parts[3])))
        total = part if total is None else total + part
    g_out[...] = total
    x_copy.wait()
    xh_out[...] = x_v[pl.ds(half * core, half), :] + x_in[...]


def gather(at):
    ncol, local_rows = at.shape
    nch = local_rows // CH
    f32 = jnp.float32
    vm, anys = pl.BlockSpec(memory_space=pltpu.VMEM), pl.BlockSpec(memory_space=pl.ANY)
    dma = pltpu.SemaphoreType.DMA
    return pl.pallas_call(
        gather_kernel,
        out_shape=(jax.ShapeDtypeStruct((nch, ncol, CH), f32), jax.ShapeDtypeStruct((nch, PANELS, BW, CH), f32), jax.ShapeDtypeStruct((ncol // 2, NC), f32),
                   jax.ShapeDtypeStruct((NC, NC), f32), jax.ShapeDtypeStruct((NC, NC), f32), jax.ShapeDtypeStruct((ncol, NC), f32)),
        in_specs=[anys],
        out_specs=(vm,) * 6,
        scratch_shapes=[pltpu.VMEM((nch, PANELS, BW, CH), f32), pltpu.VMEM((ncol, NC), f32),
                        pltpu.VMEM((NC, NC), f32), pltpu.VMEM((3, NC, NC), f32), pltpu.VMEM((ncol // 2, NC), f32),
                        pltpu.VMEM((ncol, NC), f32), pltpu.VMEM((PANELS, BW, NC), f32),
                        dma((nch,)), dma((nch,)), dma((nch, 4)), dma((nch,)), dma((nch, 4)), dma, dma((4,)), dma, dma((4,)), dma,
                        dma((3,)), dma((3,)), dma, dma],
        compiler_params=pltpu.CompilerParams(collective_id=0, has_side_effects=True, vmem_limit_bytes=GATHER_VMEM),
        name="gather",
    )(at)


def split3(x):
    hi = x.astype(jnp.bfloat16)
    rem = x - hi.astype(jnp.float32)
    mid = rem.astype(jnp.bfloat16)
    lo = (rem - mid.astype(jnp.float32)).astype(jnp.bfloat16)
    return hi, mid, lo


def store_split(dst, rows, z):
    zh, zm, zl = split3(z)
    for i, part in enumerate((zh, zm, zh, zm, zh, zl)):
        dst[rows, i * NC:(i + 1) * NC] = part


def update_kernel(a_ref, pt_ref, x0_ref, x1_ref, x2_ref, x3_ref, head_ref, rit_ref, nmat_ref, uit_ref, facet_ref, out_ref, z_v, top_v):
    step = pl.program_id(0)
    q = lax.axis_index('col')
    r = lax.axis_index('row')
    ncol = head_ref.shape[0]
    half = ncol // 2

    @pl.when(step == 0)
    def _():
        core = r % 2
        rit = rit_ref[...]
        nmat = nmat_ref[...]
        mine = pl.multiple_of(half * core, half)
        other = pl.multiple_of(half * (1 - core), half)
        for lo, xa, xb in ((mine, x0_ref, x1_ref), (other, x2_ref, x3_ref)):
            r12t = dot_nt(xa[...] + xb[...], rit)
            top_v[pl.ds(lo, half), :] = r12t
            store_split(z_v, pl.ds(lo, half), dot_nn(head_ref[pl.ds(lo, half), :] - r12t, nmat))
        own = pl.ds(pl.multiple_of(q * BW, BW), BW)
        top_v[0:BW, :] = facet_ref[own, :]
        store_split(z_v, pl.ds(0, BW), -uit_ref[own, :])

    ph, pm, plo = split3(pt_ref[step].reshape(NC, CH))
    wide = jnp.concatenate([ph, pm, pm, ph, plo, ph], axis=0)
    prod = lax.dot_general(z_v[...], wide, (((1,), (0,)), ((), ())), preferred_element_type=jnp.float32)
    out_ref[BW:, :] = a_ref[step, BW:, :] - prod[BW:]
    out_ref[0:BW, :] = -prod[0:BW]

    @pl.when(jnp.logical_and(step == 0, r == 0))
    def _():
        out_ref[:, 0:NC] = top_v[...]


def update(a, pt, xs, head, rit, nmat, uit, facet):
    nch, ncol, _ = a.shape
    vm = pl.BlockSpec(memory_space=pltpu.VMEM)
    return pl.pallas_call(
        update_kernel,
        grid=(nch,),
        out_shape=jax.ShapeDtypeStruct((ncol, nch * CH), jnp.float32),
        in_specs=[vm] * 11,
        out_specs=pl.BlockSpec((ncol, CH), lambda i: (0, i)),
        scratch_shapes=[pltpu.VMEM((ncol, 6 * NC), jnp.bfloat16), pltpu.VMEM((ncol, NC), jnp.float32)],
        compiler_params=pltpu.CompilerParams(dimension_semantics=("arbitrary",), vmem_limit_bytes=UPDATE_VMEM),
        name="update",
    )(a, pt, *xs, head, rit, nmat, uit, facet)


def solution(mesh):
    block_spec = P(('batch', 'row'), 'col', None)

    def device_fn(a_local):
        local_rows, local_blocks, bw = a_local.shape
        ncol = local_blocks * bw
        at = a_local.transpose(1, 2, 0).reshape(ncol, local_rows)
        a, pt, xh, gram, ptop, head = gather(at)
        x1, x2, x3 = [lax.ppermute(xh, 'row', [(i, i ^ b) for i in range(4)]) for b in (2, 1, 3)]
        facet, tfac, tau, rit, nmat, uit = factor(gram, ptop)
        out = update(a, pt, (xh, x1, x2, x3), head, rit, nmat, uit, facet)
        a_out = out.reshape(local_blocks, bw, local_rows).transpose(2, 0, 1)
        return a_out, tau.reshape(NC), tfac

    return jax.shard_map(device_fn, mesh=mesh, in_specs=(block_spec,), out_specs=(block_spec, P('batch'), P('batch', None, None)), check_vma=False)
```

```python
import functools
import jax
import jax.numpy as jnp
from jax import lax
from jax.experimental import pallas as pl
from jax.experimental.pallas import tpu as pltpu
from jax.sharding import PartitionSpec as P

PANELS = 4
BW = 32
NC = PANELS * BW
CH = 512
UPDATE_VMEM = 32 * 1024 * 1024
GATHER_VMEM = 32 * 1024 * 1024
AHEAD = 3
HIGHEST = lax.Precision.HIGHEST
MESH = pl.DeviceIdType.MESH


def dot_nn(x, y):
    return lax.dot_general(x, y, (((1,), (0,)), ((), ())), precision=HIGHEST, preferred_element_type=jnp.float32)


def dot_nt(x, y):
    return lax.dot_general(x, y, (((1,), (1,)), ((), ())), precision=HIGHEST, preferred_element_type=jnp.float32)


def dot_tn(x, y):
    return lax.dot_general(x, y, (((0,), (0,)), ((), ())), precision=HIGHEST, preferred_element_type=jnp.float32)


def split3(x):
    hi = x.astype(jnp.bfloat16)
    rem = x - hi.astype(jnp.float32)
    mid = rem.astype(jnp.bfloat16)
    lo = (rem - mid.astype(jnp.float32)).astype(jnp.bfloat16)
    return hi, mid, lo


def outer48(x, y):
    xh, xm, xl = [p.astype(jnp.float32) for p in split3(x)]
    yh, ym, yl = [p.astype(jnp.float32) for p in split3(y)]
    left = jnp.concatenate([xh, xm, xh, xm, xh, xl], axis=0).astype(jnp.bfloat16)
    right = jnp.concatenate([yh, ym, ym, yh, yl, yh], axis=0).astype(jnp.bfloat16)
    return lax.dot_general(left, right, (((0,), (0,)), ((), ())), preferred_element_type=jnp.float32)


def factor_kernel(g_ref, ptop_ref, facet_ref, tau_ref, tau8_ref, rit_ref, uit_ref, u_ref, li_ref, gr_v, bl_v, te_v, r_v, lt_v):
    nt = NC // 8
    lane = lax.broadcasted_iota(jnp.int32, (8, NC), 1)
    sub = lax.broadcasted_iota(jnp.int32, (8, NC), 0)
    rows = lax.broadcasted_iota(jnp.int32, (NC, NC), 0)
    cols = lax.broadcasted_iota(jnp.int32, (NC, NC), 1)
    eye = jnp.where(rows == cols, 1.0, 0.0)

    def row_of(tile, s):
        return jnp.broadcast_to(tile[s:s + 1, :], (8, NC))

    def col_of(tile, k):
        return jnp.broadcast_to(tile[:, k:k + 1], (8, NC))

    gr_v[:, 0:NC] = g_ref[...]
    bl_v[:, 0:NC] = ptop_ref[...].T
    te_v[:, 0:NC] = ptop_ref[...]
    for ref in (gr_v, bl_v, te_v):
        ref[:, NC:2 * NC] = eye
    tau_row = jnp.zeros((8, NC), jnp.float32)
    gr, bl, te = gr_v[0:8, :], bl_v[0:8, :], te_v[0:8, :]
    for block in range(nt):
        o = 8 * block
        gd, rid = gr[:, 0:NC], gr[:, NC:]
        bd, lid = bl[:, 0:NC], bl[:, NC:]
        cg = [col_of(gd, o + s) for s in range(8)]
        cb = [col_of(bd, o + s) for s in range(8)]
        bt = [row_of(te[:, 0:NC], s) for s in range(8)]
        e = [row_of(te[:, NC:], s) for s in range(8)]
        zero = jnp.zeros((8, NC), jnp.float32)
        r_b = ri_b = u_b = li_b = l_b = y_b = neg = zero
        for s in range(8):
            k = o + s
            diag = row_of(cg[s], s)
            rs = lax.rsqrt(diag)
            norm = diag * rs
            alpha = row_of(cb[s], s)
            sgn = jnp.where(alpha >= 0.0, 1.0, -1.0)
            beta = -sgn * norm
            inv = 1.0 / (alpha - beta)
            fg = cg[s] * rs
            fb = cb[s] * inv
            lrow = jnp.where(lane > k, bt[s] * inv, 0.0)
            yrow = e[s] * inv
            for j in range(s + 1, 8):
                rj = row_of(fg, j)
                uj = row_of(cb[j], s) + sgn * rj
                cg[j] = cg[j] - fg * rj
                cb[j] = cb[j] - fb * uj
                bt[j] = bt[j] - lrow * uj
                e[j] = e[j] - yrow * uj
            rrow = jnp.where(lane >= k, row_of(gd, s) * rs, 0.0)
            rirow = row_of(rid, s) * rs
            lirow = row_of(lid, s)
            urow = jnp.where(lane >= k, row_of(bd, s) + sgn * rrow, 0.0)
            gd = gd - fg * rrow
            rid = rid - fg * rirow
            bd = bd - fb * urow
            lid = lid - fb * lirow
            here = sub == s
            r_b = jnp.where(here, rrow, r_b)
            ri_b = jnp.where(here, rirow, ri_b)
            u_b = jnp.where(here, urow, u_b)
            li_b = jnp.where(here, lirow, li_b)
            l_b = jnp.where(here, lrow, l_b)
            y_b = jnp.where(here, yrow, y_b)
            neg = jnp.where(here, -sgn, neg)
            tau_row = jnp.where(lane == k, (beta - alpha) / beta, tau_row)
        tile = slice(o, o + 8)
        r_v[tile, :] = r_b * neg
        rit_ref[tile, :] = ri_b * neg
        u_ref[tile, :] = u_b
        li_ref[tile, :] = li_b
        lt_v[tile, :] = l_b
        uit_ref[tile, :] = y_b
        if block + 1 < nt:
            new = []
            for ref, x, y in ((gr_v, r_b, (r_b, ri_b)), (bl_v, l_b, (u_b, li_b)), (te_v, u_b, (l_b, y_b))):
                prod = outer48(x, jnp.concatenate(y, axis=1))
                new.append(ref[o + 8:o + 16, :] - prod[o + 8:o + 16])
                if block + 2 < nt:
                    ref[o + 16:, :] = ref[o + 16:, :] - prod[o + 16:]
            gr, bl, te = new
    tau_ref[...] = tau_row[0:1]
    tau8_ref[...] = tau_row
    facet_ref[...] = jnp.where(cols > rows, lt_v[...], r_v[...].T)


def finish_kernel(tau8_ref, rit_ref, uit_ref, u_ref, li_ref, tfac_ref, nmat_ref):
    limat = li_ref[...]
    nmat_ref[...] = dot_tn(limat, uit_ref[...])
    tful = -dot_nt(dot_nt(u_ref[...], rit_ref[...]), limat)
    rows = lax.broadcasted_iota(jnp.int32, (NC, NC), 0)
    cols = lax.broadcasted_iota(jnp.int32, (NC, NC), 1)
    tful = jnp.where(cols > rows, tful, 0.0)
    tful = jnp.where(cols == rows, jnp.broadcast_to(tau8_ref[0:1, :], (NC, NC)), tful)
    for j in range(PANELS):
        tfac_ref[j] = tful[j * BW:(j + 1) * BW, j * BW:(j + 1) * BW]


def factor(gram, ptop):
    sq = jax.ShapeDtypeStruct((NC, NC), jnp.float32)
    vm = pl.BlockSpec(memory_space=pltpu.VMEM)
    tau = jax.ShapeDtypeStruct((1, NC), jnp.float32)
    return pl.pallas_call(
        factor_kernel,
        out_shape=(sq, tau, jax.ShapeDtypeStruct((8, NC), jnp.float32), sq, sq, sq, sq),
        in_specs=[vm] * 2,
        out_specs=(vm,) * 7,
        scratch_shapes=[pltpu.VMEM((NC, 2 * NC), jnp.float32)] * 3 + [pltpu.VMEM((NC, NC), jnp.float32)] * 2,
        compiler_params=pltpu.CompilerParams(vmem_limit_bytes=8 * 1024 * 1024),
        cost_estimate=pl.CostEstimate(flops=1_000_000_000, bytes_accessed=600_000, transcendentals=0),
        name="factor",
    )(gram, ptop)


def finish(tau8, rit, uit, u, li):
    vm = pl.BlockSpec(memory_space=pltpu.VMEM)
    return pl.pallas_call(
        finish_kernel,
        out_shape=(jax.ShapeDtypeStruct((PANELS, BW, BW), jnp.float32), jax.ShapeDtypeStruct((NC, NC), jnp.float32)),
        in_specs=[vm] * 5,
        out_specs=(vm,) * 2,
        compiler_params=pltpu.CompilerParams(vmem_limit_bytes=4 * 1024 * 1024),
        cost_estimate=pl.CostEstimate(flops=300_000_000, bytes_accessed=400_000, transcendentals=0),
        name="finish",
    )(tau8, rit, uit, u, li)


def gather_kernel(at_ref, a_v, pt_out, xh_out, g_out, ptop_out, head_out,
                  pt_v, x_v, g_v, g_in, x_in, head_v, ptop_v,
                  a_sem, own_sem, send, fwd, recv, h_sem, hsend, hrecv, psend, precv, gsend, grecv, xsend, xrecv):
    ncol, local_rows = at_ref.shape
    nch = local_rows // CH
    half = ncol // 2
    q = lax.axis_index('col')
    r = lax.axis_index('row')
    last = lax.axis_size('col') - 1

    def own_load(c):
        return pltpu.make_async_copy(at_ref.at[pl.ds(0, BW), pl.ds(c * CH, CH)], pt_v.at[c, q], own_sem.at[c])

    def a_load(c):
        return pltpu.make_async_copy(at_ref.at[:, pl.ds(c * CH, CH)], a_v.at[c], a_sem.at[c])

    def hop(c, j, to, sem):
        return pltpu.make_async_remote_copy(
            src_ref=pt_v.at[c, j], dst_ref=pt_v.at[c, j], send_sem=sem, recv_sem=recv.at[c, j],
            device_id={'col': to}, device_id_type=MESH)

    routes = ((q + 2, q + 2 <= last, 0), (q - 2, q >= 2, 1), (q + 1, q < last, 2), (q - 1, q > 0, 3))

    def send_own(c):
        own_load(c).wait()
        for to, valid, slot in routes:
            @pl.when(valid)
            def _():
                hop(c, q, to, send.at[c, slot]).start()

    def head_send(p):
        return pltpu.make_async_remote_copy(
            src_ref=at_ref.at[:, pl.ds(0, NC)], dst_ref=head_v, send_sem=hsend.at[p], recv_sem=hrecv,
            device_id={'row': p}, device_id_type=MESH)

    def ptop_send(p):
        return pltpu.make_async_remote_copy(
            src_ref=pt_v.at[0, :, :, pl.ds(0, NC)], dst_ref=ptop_v, send_sem=psend.at[p], recv_sem=precv,
            device_id={'row': p}, device_id_type=MESH)

    for c in range(nch):
        own_load(c).start()
    for c in range(nch):
        a_load(c).start()

    barrier = pltpu.get_barrier_semaphore()

    for to, valid, _ in routes:
        @pl.when(valid)
        def _():
            pl.semaphore_signal(barrier, inc=1, device_id={'col': to}, device_id_type=MESH)

    for d in range(1, 4):
        pl.semaphore_signal(barrier, inc=1, device_id={'row': (r + d) % 4}, device_id_type=MESH)
    inner = jnp.logical_and(q > 0, q < last)

    @pl.when(inner)
    def _():
        pl.semaphore_wait(barrier, 6)

    @pl.when(jnp.logical_not(inner))
    def _():
        pl.semaphore_wait(barrier, 5)

    for c in range(min(AHEAD, nch)):
        send_own(c)

    head_local = pltpu.make_async_copy(at_ref.at[:, pl.ds(0, NC)], head_v, h_sem)

    @pl.when(r == 0)
    def _():
        for p in range(1, 4):
            head_send(p).start()
        head_local.start()

    x_v[...] = jnp.zeros_like(x_v)
    g_v[...] = jnp.zeros_like(g_v)

    g_copies = []
    for d in range(1, 4):
        g_copies.append(pltpu.make_async_remote_copy(
            src_ref=g_v, dst_ref=g_in.at[d - 1], send_sem=gsend.at[d - 1], recv_sem=grecv.at[d - 1],
            device_id={'row': (r + d) % 4}, device_id_type=MESH))

    def chunk(c, carry):
        @pl.when(c + AHEAD < nch)
        def _():
            send_own(c + AHEAD)

        for d in range(1, 4):
            @pl.when(q >= d)
            def _():
                hop(c, q - d, q, fwd.at[c]).wait_recv()

            @pl.when(q + d <= last)
            def _():
                hop(c, q + d, q, fwd.at[c]).wait_recv()

            if d == 2:
                @pl.when(q == last - 1)
                def _():
                    hop(c, 0, q + 1, fwd.at[c]).start()

                @pl.when(q == 1)
                def _():
                    hop(c, last, q - 1, fwd.at[c]).start()

        pt_out[c] = pt_v[c]

        @pl.when(jnp.logical_and(c == 0, r == 0))
        def _():
            for p in range(1, 4):
                ptop_send(p).start()
            for j in range(PANELS):
                ptop_out[j * BW:(j + 1) * BW, :] = pt_v[0, j, :, 0:NC]

        a_load(c).wait()
        p = pt_v[c].reshape(NC, CH)
        g_v[...] += dot_nt(p, p)

        @pl.when(c == nch - 1)
        def _():
            for g_copy in g_copies:
                g_copy.start()

        x_v[...] += dot_nt(a_v[c], p)
        return carry

    lax.fori_loop(0, nch, chunk, 0)

    core = r % 2
    mate = r + 1 - 2 * core
    x_copy = pltpu.make_async_remote_copy(
        src_ref=x_v.at[pl.ds(half * (1 - core), half)], dst_ref=x_in, send_sem=xsend, recv_sem=xrecv,
        device_id={'row': mate}, device_id_type=MESH)
    x_copy.start()
    @pl.when(r == 0)
    def _():
        for p in range(1, 4):
            head_send(p).wait_send()
            ptop_send(p).wait_send()
        head_local.wait()

    @pl.when(r > 0)
    def _():
        head_send(0).wait_recv()
        ptop_send(0).wait_recv()
        for j in range(PANELS):
            ptop_out[j * BW:(j + 1) * BW, :] = ptop_v[j]

    head_out[...] = head_v[...]

    def drain(c, carry):
        for to, valid, slot in routes:
            @pl.when(valid)
            def _():
                hop(c, q, to, send.at[c, slot]).wait_send()

        @pl.when(inner)
        def _():
            hop(c, q, q, fwd.at[c]).wait_send()

        return carry

    lax.fori_loop(0, nch, drain, 0)
    for g_copy in g_copies:
        g_copy.wait()
    parts = [g_v[...]] + [g_in[d - 1] for d in range(1, 4)]
    total = None
    for row in range(4):
        dist = (r - row + 4) % 4
        part = jnp.where(dist == 0, parts[0], jnp.where(dist == 1, parts[1], jnp.where(dist == 2, parts[2], parts[3])))
        total = part if total is None else total + part
    g_out[...] = total
    x_copy.wait()
    xh_out[...] = x_v[pl.ds(half * core, half), :] + x_in[...]


def gather(at):
    ncol, local_rows = at.shape
    nch = local_rows // CH
    f32 = jnp.float32
    vm, anys = pl.BlockSpec(memory_space=pltpu.VMEM), pl.BlockSpec(memory_space=pl.ANY)
    dma = pltpu.SemaphoreType.DMA
    return pl.pallas_call(
        gather_kernel,
        out_shape=(jax.ShapeDtypeStruct((nch, ncol, CH), f32), jax.ShapeDtypeStruct((nch, PANELS, BW, CH), f32), jax.ShapeDtypeStruct((ncol // 2, NC), f32),
                   jax.ShapeDtypeStruct((NC, NC), f32), jax.ShapeDtypeStruct((NC, NC), f32), jax.ShapeDtypeStruct((ncol, NC), f32)),
        in_specs=[anys],
        out_specs=(vm,) * 6,
        scratch_shapes=[pltpu.VMEM((nch, PANELS, BW, CH), f32), pltpu.VMEM((ncol, NC), f32),
                        pltpu.VMEM((NC, NC), f32), pltpu.VMEM((3, NC, NC), f32), pltpu.VMEM((ncol // 2, NC), f32),
                        pltpu.VMEM((ncol, NC), f32), pltpu.VMEM((PANELS, BW, NC), f32),
                        dma((nch,)), dma((nch,)), dma((nch, 4)), dma((nch,)), dma((nch, 4)), dma, dma((4,)), dma, dma((4,)), dma,
                        dma((3,)), dma((3,)), dma, dma],
        compiler_params=pltpu.CompilerParams(collective_id=0, has_side_effects=True, vmem_limit_bytes=GATHER_VMEM),
        name="gather",
    )(at)


def store_split(dst, rows, z):
    zh, zm, zl = split3(z)
    for i, part in enumerate((zh, zm, zh, zm, zh, zl)):
        dst[rows, i * NC:(i + 1) * NC] = part


def update_kernel(a_ref, pt_ref, x0_ref, x1_ref, x2_ref, x3_ref, head_ref, rit_ref, nmat_ref, uit_ref, facet_ref, out_ref, z_v, top_v):
    step = pl.program_id(0)
    q = lax.axis_index('col')
    r = lax.axis_index('row')
    ncol = head_ref.shape[0]
    half = ncol // 2

    @pl.when(step == 0)
    def _():
        core = r % 2
        rit = rit_ref[...]
        nmat = nmat_ref[...]
        mine = pl.multiple_of(half * core, half)
        other = pl.multiple_of(half * (1 - core), half)
        for lo, xa, xb in ((mine, x0_ref, x1_ref), (other, x2_ref, x3_ref)):
            r12t = dot_nt(xa[...] + xb[...], rit)
            top_v[pl.ds(lo, half), :] = r12t
            store_split(z_v, pl.ds(lo, half), dot_nn(head_ref[pl.ds(lo, half), :] - r12t, nmat))
        own = pl.ds(pl.multiple_of(q * BW, BW), BW)
        top_v[0:BW, :] = facet_ref[own, :]
        store_split(z_v, pl.ds(0, BW), -uit_ref[own, :])

    ph, pm, plo = split3(pt_ref[step].reshape(NC, CH))
    wide = jnp.concatenate([ph, pm, pm, ph, plo, ph], axis=0)
    prod = lax.dot_general(z_v[...], wide, (((1,), (0,)), ((), ())), preferred_element_type=jnp.float32)
    out_ref[BW:, :] = a_ref[step, BW:, :] - prod[BW:]
    out_ref[0:BW, :] = -prod[0:BW]

    @pl.when(jnp.logical_and(step == 0, r == 0))
    def _():
        out_ref[:, 0:NC] = top_v[...]


def update(a, pt, xs, head, rit, nmat, uit, facet):
    nch, ncol, _ = a.shape
    vm = pl.BlockSpec(memory_space=pltpu.VMEM)
    return pl.pallas_call(
        update_kernel,
        grid=(nch,),
        out_shape=jax.ShapeDtypeStruct((ncol, nch * CH), jnp.float32),
        in_specs=[vm] * 11,
        out_specs=pl.BlockSpec((ncol, CH), lambda i: (0, i)),
        scratch_shapes=[pltpu.VMEM((ncol, 6 * NC), jnp.bfloat16), pltpu.VMEM((ncol, NC), jnp.float32)],
        compiler_params=pltpu.CompilerParams(dimension_semantics=("arbitrary",), vmem_limit_bytes=UPDATE_VMEM),
        name="update",
    )(a, pt, *xs, head, rit, nmat, uit, facet)


def solution(mesh):
    block_spec = P(('batch', 'row'), 'col', None)

    def device_fn(a_local):
        local_rows, local_blocks, bw = a_local.shape
        ncol = local_blocks * bw
        at = a_local.transpose(1, 2, 0).reshape(ncol, local_rows)
        a, pt, xh, gram, ptop, head = gather(at)
        x1, x2 = [lax.ppermute(xh, 'row', [(i, i ^ b) for i in range(4)]) for b in (2, 1)]
        facet, tau, tau8, rit, uit, u, li = factor(gram, ptop)
        x1, u = lax.optimization_barrier((x1, u))
        x3 = lax.ppermute(x1, 'row', [(i, i ^ 1) for i in range(4)])
        tfac, nmat = finish(tau8, rit, uit, u, li)
        out = update(a, pt, (xh, x1, x2, x3), head, rit, nmat, uit, facet)
        a_out = out.reshape(local_blocks, bw, local_rows).transpose(2, 0, 1)
        return a_out, tau.reshape(NC), tfac

    return jax.shard_map(device_fn, mesh=mesh, in_specs=(block_spec,), out_specs=(block_spec, P('batch'), P('batch', None, None)), check_vma=False)
```

```python
import functools
import jax
import jax.numpy as jnp
from jax import lax
from jax.experimental import pallas as pl
from jax.experimental.pallas import tpu as pltpu
from jax.sharding import PartitionSpec as P

PANELS = 4
BW = 32
NC = PANELS * BW
CH = 512
UPDATE_VMEM = 32 * 1024 * 1024
GATHER_VMEM = 32 * 1024 * 1024
HIGHEST = lax.Precision.HIGHEST
MESH = pl.DeviceIdType.MESH


def dot_nt(x, y):
    return lax.dot_general(x, y, (((1,), (1,)), ((), ())), precision=HIGHEST, preferred_element_type=jnp.float32)


def split3(x):
    hi = x.astype(jnp.bfloat16)
    rem = x - hi.astype(jnp.float32)
    mid = rem.astype(jnp.bfloat16)
    lo = (rem - mid.astype(jnp.float32)).astype(jnp.bfloat16)
    return hi, mid, lo


def stack6(x, axis, order):
    parts = split3(x)
    return jnp.concatenate([parts[i] for i in order], axis=axis)


LEFT, RIGHT = (0, 1, 0, 1, 0, 2), (0, 1, 1, 0, 2, 0)


def dot6(x, y, dims):
    left = stack6(x, dims[0], LEFT)
    right = stack6(y, dims[1], RIGHT)
    return lax.dot_general(left, right, (((dims[0],), (dims[1],)), ((), ())), preferred_element_type=jnp.float32)


def outer48(x, y):
    xh, xm, xl = [p.astype(jnp.float32) for p in split3(x)]
    yh, ym, yl = [p.astype(jnp.float32) for p in split3(y)]
    left = jnp.concatenate([xh, xm, xh, xm, xh, xl], axis=0).astype(jnp.bfloat16)
    right = jnp.concatenate([yh, ym, ym, yh, yl, yh], axis=0).astype(jnp.bfloat16)
    return lax.dot_general(left, right, (((0,), (0,)), ((), ())), preferred_element_type=jnp.float32)


def factor_kernel(g_ref, ptop_ref, facet_ref, tau_ref, tau8_ref, rit_ref, uit_ref, u_ref, li_ref, gr_v, bl_v, te_v, r_v, lt_v):
    nt = NC // 8
    lane = lax.broadcasted_iota(jnp.int32, (8, NC), 1)
    sub = lax.broadcasted_iota(jnp.int32, (8, NC), 0)
    rows = lax.broadcasted_iota(jnp.int32, (NC, NC), 0)
    cols = lax.broadcasted_iota(jnp.int32, (NC, NC), 1)
    eye = jnp.where(rows == cols, 1.0, 0.0)

    def row_of(tile, s):
        return jnp.broadcast_to(tile[s:s + 1, :], (8, NC))

    def col_of(tile, k):
        return jnp.broadcast_to(tile[:, k:k + 1], (8, NC))

    gr_v[:, 0:NC] = g_ref[...]
    bl_v[:, 0:NC] = ptop_ref[...].T
    te_v[:, 0:NC] = ptop_ref[...]
    for ref in (gr_v, bl_v, te_v):
        ref[:, NC:2 * NC] = eye
    tau_row = jnp.zeros((8, NC), jnp.float32)
    gr, bl, te = gr_v[0:8, :], bl_v[0:8, :], te_v[0:8, :]
    for block in range(nt):
        o = 8 * block
        gd, rid = gr[:, 0:NC], gr[:, NC:]
        bd, lid = bl[:, 0:NC], bl[:, NC:]
        cg = [col_of(gd, o + s) for s in range(8)]
        cb = [col_of(bd, o + s) for s in range(8)]
        bt = [row_of(te[:, 0:NC], s) for s in range(8)]
        e = [row_of(te[:, NC:], s) for s in range(8)]
        zero = jnp.zeros((8, NC), jnp.float32)
        r_b = ri_b = u_b = li_b = l_b = y_b = neg = zero
        for s in range(8):
            k = o + s
            diag = row_of(cg[s], s)
            rs = lax.rsqrt(diag)
            norm = diag * rs
            alpha = row_of(cb[s], s)
            sgn = jnp.where(alpha >= 0.0, 1.0, -1.0)
            beta = -sgn * norm
            inv = 1.0 / (alpha - beta)
            fg = cg[s] * rs
            fb = cb[s] * inv
            lrow = jnp.where(lane > k, bt[s] * inv, 0.0)
            yrow = e[s] * inv
            for j in range(s + 1, 8):
                rj = row_of(fg, j)
                uj = row_of(cb[j], s) + sgn * rj
                cg[j] = cg[j] - fg * rj
                cb[j] = cb[j] - fb * uj
                bt[j] = bt[j] - lrow * uj
                e[j] = e[j] - yrow * uj
            rrow = jnp.where(lane >= k, row_of(gd, s) * rs, 0.0)
            rirow = row_of(rid, s) * rs
            lirow = row_of(lid, s)
            urow = jnp.where(lane >= k, row_of(bd, s) + sgn * rrow, 0.0)
            gd = gd - fg * rrow
            rid = rid - fg * rirow
            bd = bd - fb * urow
            lid = lid - fb * lirow
            here = sub == s
            r_b = jnp.where(here, rrow, r_b)
            ri_b = jnp.where(here, rirow, ri_b)
            u_b = jnp.where(here, urow, u_b)
            li_b = jnp.where(here, lirow, li_b)
            l_b = jnp.where(here, lrow, l_b)
            y_b = jnp.where(here, yrow, y_b)
            neg = jnp.where(here, -sgn, neg)
            tau_row = jnp.where(lane == k, (beta - alpha) / beta, tau_row)
        tile = slice(o, o + 8)
        r_v[tile, :] = r_b * neg
        rit_ref[tile, :] = ri_b * neg
        u_ref[tile, :] = u_b
        li_ref[tile, :] = li_b
        lt_v[tile, :] = l_b
        uit_ref[tile, :] = y_b
        if block + 1 < nt:
            new = []
            for ref, x, y in ((gr_v, r_b, (r_b, ri_b)), (bl_v, l_b, (u_b, li_b)), (te_v, u_b, (l_b, y_b))):
                prod = outer48(x, jnp.concatenate(y, axis=1))
                new.append(ref[o + 8:o + 16, :] - prod[o + 8:o + 16])
                if block + 2 < nt:
                    ref[o + 16:, :] = ref[o + 16:, :] - prod[o + 16:]
            gr, bl, te = new
    tau_ref[...] = tau_row[0:1]
    tau8_ref[...] = tau_row
    facet_ref[...] = jnp.where(cols > rows, lt_v[...], r_v[...].T)


def finish_kernel(tau8_ref, rit_ref, uit_ref, u_ref, li_ref, tfac_ref, nmat_ref):
    limat = li_ref[...]
    nmat_ref[...] = dot6(limat.T, uit_ref[...], (1, 0))
    tful = -dot6(dot6(u_ref[...], rit_ref[...], (1, 1)), limat, (1, 1))
    rows = lax.broadcasted_iota(jnp.int32, (NC, NC), 0)
    cols = lax.broadcasted_iota(jnp.int32, (NC, NC), 1)
    tful = jnp.where(cols > rows, tful, 0.0)
    tful = jnp.where(cols == rows, jnp.broadcast_to(tau8_ref[0:1, :], (NC, NC)), tful)
    for j in range(PANELS):
        tfac_ref[j] = tful[j * BW:(j + 1) * BW, j * BW:(j + 1) * BW]


def factor(gram, ptop):
    sq = jax.ShapeDtypeStruct((NC, NC), jnp.float32)
    vm = pl.BlockSpec(memory_space=pltpu.VMEM)
    tau = jax.ShapeDtypeStruct((1, NC), jnp.float32)
    return pl.pallas_call(
        factor_kernel,
        out_shape=(sq, tau, jax.ShapeDtypeStruct((8, NC), jnp.float32), sq, sq, sq, sq),
        in_specs=[vm] * 2,
        out_specs=(vm,) * 7,
        scratch_shapes=[pltpu.VMEM((NC, 2 * NC), jnp.float32)] * 3 + [pltpu.VMEM((NC, NC), jnp.float32)] * 2,
        compiler_params=pltpu.CompilerParams(vmem_limit_bytes=8 * 1024 * 1024),
        cost_estimate=pl.CostEstimate(flops=1_000_000_000, bytes_accessed=600_000, transcendentals=0),
        name="factor",
    )(gram, ptop)


def finish(tau8, rit, uit, u, li):
    vm = pl.BlockSpec(memory_space=pltpu.VMEM)
    return pl.pallas_call(
        finish_kernel,
        out_shape=(jax.ShapeDtypeStruct((PANELS, BW, BW), jnp.float32), jax.ShapeDtypeStruct((NC, NC), jnp.float32)),
        in_specs=[vm] * 5,
        out_specs=(vm,) * 2,
        compiler_params=pltpu.CompilerParams(vmem_limit_bytes=4 * 1024 * 1024),
        cost_estimate=pl.CostEstimate(flops=300_000_000, bytes_accessed=400_000, transcendentals=0),
        name="finish",
    )(tau8, rit, uit, u, li)


def gather_kernel(at_ref, a_v, pt_out, xh_out, g_out, ptop_out, head_out,
                  pt_v, x_v, g_v, g_in, x_in, head_v, ptop_v,
                  a_sem, own_sem, send, fwd, recv, h_sem, hsend, hrecv, psend, precv, gsend, grecv, xsend, xrecv):
    ncol, local_rows = at_ref.shape
    nch = local_rows // CH
    half = ncol // 2
    q = lax.axis_index('col')
    r = lax.axis_index('row')
    last = lax.axis_size('col') - 1

    def own_load(c):
        return pltpu.make_async_copy(at_ref.at[pl.ds(0, BW), pl.ds(c * CH, CH)], pt_v.at[c, q], own_sem.at[c])

    def a_load(c):
        return pltpu.make_async_copy(at_ref.at[:, pl.ds(c * CH, CH)], a_v.at[c], a_sem.at[c])

    def hop(c, j, to, sem):
        return pltpu.make_async_remote_copy(
            src_ref=pt_v.at[c, j], dst_ref=pt_v.at[c, j], send_sem=sem, recv_sem=recv.at[c, j],
            device_id={'col': to}, device_id_type=MESH)

    at_end = jnp.logical_or(q == 0, q == last)
    inward = jnp.where(q == 0, 1, -1)
    routes = ((q + 2 * inward, at_end, 0), (q + inward, at_end, 1), (q + 1, jnp.logical_not(at_end), 0), (q - 1, jnp.logical_not(at_end), 1))

    def send_own(c):
        own_load(c).wait()
        for to, valid, slot in routes:
            @pl.when(valid)
            def _():
                hop(c, q, to, send.at[c, slot]).start()

    def head_send(p):
        return pltpu.make_async_remote_copy(
            src_ref=at_ref.at[:, pl.ds(0, NC)], dst_ref=head_v, send_sem=hsend.at[p], recv_sem=hrecv,
            device_id={'row': p}, device_id_type=MESH)

    def ptop_send(p):
        return pltpu.make_async_remote_copy(
            src_ref=pt_v.at[0, :, :, pl.ds(0, NC)], dst_ref=ptop_v, send_sem=psend.at[p], recv_sem=precv,
            device_id={'row': p}, device_id_type=MESH)

    for c in range(nch):
        own_load(c).start()
    for c in range(nch):
        a_load(c).start()

    barrier = pltpu.get_barrier_semaphore()

    for to, valid in ((q + 2, q + 2 <= last), (q - 2, q >= 2), (q + 1, q < last), (q - 1, q > 0)):
        @pl.when(valid)
        def _():
            pl.semaphore_signal(barrier, inc=1, device_id={'col': to}, device_id_type=MESH)

    for d in range(1, 4):
        pl.semaphore_signal(barrier, inc=1, device_id={'row': (r + d) % 4}, device_id_type=MESH)
    inner = jnp.logical_not(at_end)
    outward = jnp.where(q == 1, -1, 1)

    @pl.when(inner)
    def _():
        pl.semaphore_wait(barrier, 6)

    @pl.when(jnp.logical_not(inner))
    def _():
        pl.semaphore_wait(barrier, 5)

    for c in range(nch):
        send_own(c)

    head_local = pltpu.make_async_copy(at_ref.at[:, pl.ds(0, NC)], head_v, h_sem)

    @pl.when(r == 0)
    def _():
        for p in range(1, 4):
            head_send(p).start()
        head_local.start()

    x_v[...] = jnp.zeros_like(x_v)
    g_v[...] = jnp.zeros_like(g_v)

    g_copies = []
    for d in range(1, 4):
        g_copies.append(pltpu.make_async_remote_copy(
            src_ref=g_v, dst_ref=g_in.at[d - 1], send_sem=gsend.at[d - 1], recv_sem=grecv.at[d - 1],
            device_id={'row': (r + d) % 4}, device_id_type=MESH))

    def chunk(c, carry):
        near, far = q - outward, q - 2 * outward

        @pl.when(inner)
        def _():
            hop(c, near, q, fwd.at[c, 0]).wait_recv()
            hop(c, near, q + outward, fwd.at[c, 0]).start()
            hop(c, far, q, fwd.at[c, 1]).wait_recv()
            hop(c, far, q + outward, fwd.at[c, 1]).start()
            hop(c, q + outward, q, fwd.at[c, 0]).wait_recv()

        @pl.when(at_end)
        def _():
            for d in range(1, 4):
                hop(c, q + d * inward, q, fwd.at[c, 0]).wait_recv()

        pt_out[c] = pt_v[c]

        @pl.when(jnp.logical_and(c == 0, r == 0))
        def _():
            for p in range(1, 4):
                ptop_send(p).start()
            for j in range(PANELS):
                ptop_out[j * BW:(j + 1) * BW, :] = pt_v[0, j, :, 0:NC]

        a_load(c).wait()
        p = pt_v[c].reshape(NC, CH)
        g_v[...] += dot_nt(p, p)

        @pl.when(c == nch - 1)
        def _():
            for g_copy in g_copies:
                g_copy.start()

        x_v[...] += dot_nt(a_v[c], p)
        return carry

    lax.fori_loop(0, nch, chunk, 0)

    core = r % 2
    mate = r + 1 - 2 * core
    x_copy = pltpu.make_async_remote_copy(
        src_ref=x_v.at[pl.ds(half * (1 - core), half)], dst_ref=x_in, send_sem=xsend, recv_sem=xrecv,
        device_id={'row': mate}, device_id_type=MESH)
    x_copy.start()
    @pl.when(r == 0)
    def _():
        for p in range(1, 4):
            head_send(p).wait_send()
            ptop_send(p).wait_send()
        head_local.wait()

    @pl.when(r > 0)
    def _():
        head_send(0).wait_recv()
        ptop_send(0).wait_recv()
        for j in range(PANELS):
            ptop_out[j * BW:(j + 1) * BW, :] = ptop_v[j]

    head_out[...] = head_v[...]

    def drain(c, carry):
        for to, valid, slot in routes:
            @pl.when(valid)
            def _():
                hop(c, q, to, send.at[c, slot]).wait_send()

        @pl.when(inner)
        def _():
            for slot in range(2):
                hop(c, q, q, fwd.at[c, slot]).wait_send()

        return carry

    lax.fori_loop(0, nch, drain, 0)
    for g_copy in g_copies:
        g_copy.wait()
    parts = [g_v[...]] + [g_in[d - 1] for d in range(1, 4)]
    total = None
    for row in range(4):
        dist = (r - row + 4) % 4
        part = jnp.where(dist == 0, parts[0], jnp.where(dist == 1, parts[1], jnp.where(dist == 2, parts[2], parts[3])))
        total = part if total is None else total + part
    g_out[...] = total
    x_copy.wait()
    xh_out[...] = x_v[pl.ds(half * core, half), :] + x_in[...]


def gather(at):
    ncol, local_rows = at.shape
    nch = local_rows // CH
    f32 = jnp.float32
    vm, anys = pl.BlockSpec(memory_space=pltpu.VMEM), pl.BlockSpec(memory_space=pl.ANY)
    dma = pltpu.SemaphoreType.DMA
    return pl.pallas_call(
        gather_kernel,
        out_shape=(jax.ShapeDtypeStruct((nch, ncol, CH), f32), jax.ShapeDtypeStruct((nch, PANELS, BW, CH), f32), jax.ShapeDtypeStruct((ncol // 2, NC), f32),
                   jax.ShapeDtypeStruct((NC, NC), f32), jax.ShapeDtypeStruct((NC, NC), f32), jax.ShapeDtypeStruct((ncol, NC), f32)),
        in_specs=[anys],
        out_specs=(vm,) * 6,
        scratch_shapes=[pltpu.VMEM((nch, PANELS, BW, CH), f32), pltpu.VMEM((ncol, NC), f32),
                        pltpu.VMEM((NC, NC), f32), pltpu.VMEM((3, NC, NC), f32), pltpu.VMEM((ncol // 2, NC), f32),
                        pltpu.VMEM((ncol, NC), f32), pltpu.VMEM((PANELS, BW, NC), f32),
                        dma((nch,)), dma((nch,)), dma((nch, 2)), dma((nch, 2)), dma((nch, 4)), dma, dma((4,)), dma, dma((4,)), dma,
                        dma((3,)), dma((3,)), dma, dma],
        compiler_params=pltpu.CompilerParams(collective_id=0, has_side_effects=True, vmem_limit_bytes=GATHER_VMEM),
        name="gather",
    )(at)


def update_kernel(a_ref, pt_ref, x0_ref, x1_ref, x2_ref, x3_ref, head_ref, rit_ref, nmat_ref, uit_ref, facet_ref, out_ref, z_v, top_v):
    step = pl.program_id(0)
    q = lax.axis_index('col')
    r = lax.axis_index('row')
    ncol = head_ref.shape[0]
    half = ncol // 2

    @pl.when(step == 0)
    def _():
        core = r % 2
        rit = rit_ref[...]
        nmat = nmat_ref[...]
        mine = pl.multiple_of(half * core, half)
        other = pl.multiple_of(half * (1 - core), half)
        for lo, xa, xb in ((mine, x0_ref, x1_ref), (other, x2_ref, x3_ref)):
            r12t = dot6(xa[...] + xb[...], rit, (1, 1))
            top_v[pl.ds(lo, half), :] = r12t
            z_v[pl.ds(lo, half), :] = stack6(dot6(head_ref[pl.ds(lo, half), :] - r12t, nmat, (1, 0)), 1, LEFT)
        own = pl.ds(pl.multiple_of(q * BW, BW), BW)
        top_v[0:BW, :] = facet_ref[own, :]
        z_v[0:BW, :] = stack6(-uit_ref[own, :], 1, LEFT)

    wide = stack6(pt_ref[step].reshape(NC, CH), 0, RIGHT)
    prod = lax.dot_general(z_v[...], wide, (((1,), (0,)), ((), ())), preferred_element_type=jnp.float32)
    out_ref[BW:, :] = a_ref[step, BW:, :] - prod[BW:]
    out_ref[0:BW, :] = -prod[0:BW]

    @pl.when(jnp.logical_and(step == 0, r == 0))
    def _():
        out_ref[:, 0:NC] = top_v[...]


def update(a, pt, xs, head, rit, nmat, uit, facet):
    nch, ncol, _ = a.shape
    vm = pl.BlockSpec(memory_space=pltpu.VMEM)
    return pl.pallas_call(
        update_kernel,
        grid=(nch,),
        out_shape=jax.ShapeDtypeStruct((ncol, nch * CH), jnp.float32),
        in_specs=[vm] * 11,
        out_specs=pl.BlockSpec((ncol, CH), lambda i: (0, i)),
        scratch_shapes=[pltpu.VMEM((ncol, 6 * NC), jnp.bfloat16), pltpu.VMEM((ncol, NC), jnp.float32)],
        compiler_params=pltpu.CompilerParams(dimension_semantics=("arbitrary",), vmem_limit_bytes=UPDATE_VMEM),
        name="update",
    )(a, pt, *xs, head, rit, nmat, uit, facet)


def solution(mesh):
    block_spec = P(('batch', 'row'), 'col', None)

    def device_fn(a_local):
        local_rows, local_blocks, bw = a_local.shape
        ncol = local_blocks * bw
        at = a_local.transpose(1, 2, 0).reshape(ncol, local_rows)
        a, pt, xh, gram, ptop, head = gather(at)
        x1, x2 = [lax.ppermute(xh, 'row', [(i, i ^ b) for i in range(4)]) for b in (2, 1)]
        facet, tau, tau8, rit, uit, u, li = factor(gram, ptop)
        x1, u = lax.optimization_barrier((x1, u))
        x3 = lax.ppermute(x1, 'row', [(i, i ^ 1) for i in range(4)])
        tfac, nmat = finish(tau8, rit, uit, u, li)
        out = update(a, pt, (xh, x1, x2, x3), head, rit, nmat, uit, facet)
        a_out = out.reshape(local_blocks, bw, local_rows).transpose(2, 0, 1)
        return a_out, tau.reshape(NC), tfac

    return jax.shard_map(device_fn, mesh=mesh, in_specs=(block_spec,), out_specs=(block_spec, P('batch'), P('batch', None, None)), check_vma=False)
```

```python
import functools
import jax
import jax.numpy as jnp
from jax import lax
from jax.experimental import pallas as pl
from jax.experimental.pallas import tpu as pltpu
from jax.sharding import PartitionSpec as P

PANELS = 4
BW = 32
NC = PANELS * BW
CH = 512
UPDATE_VMEM = 32 * 1024 * 1024
GATHER_VMEM = 32 * 1024 * 1024
HIGHEST = lax.Precision.HIGHEST
MESH = pl.DeviceIdType.MESH


def dot_nt(x, y):
    return lax.dot_general(x, y, (((1,), (1,)), ((), ())), precision=HIGHEST, preferred_element_type=jnp.float32)


def split3(x):
    hi = x.astype(jnp.bfloat16)
    rem = x - hi.astype(jnp.float32)
    mid = rem.astype(jnp.bfloat16)
    lo = (rem - mid.astype(jnp.float32)).astype(jnp.bfloat16)
    return hi, mid, lo


def stack6(x, axis, order):
    parts = split3(x)
    return jnp.concatenate([parts[i] for i in order], axis=axis)


LEFT, RIGHT = (0, 1, 0, 1, 0, 2), (0, 1, 1, 0, 2, 0)


def dot6(x, y, dims):
    left = stack6(x, dims[0], LEFT)
    right = stack6(y, dims[1], RIGHT)
    return lax.dot_general(left, right, (((dims[0],), (dims[1],)), ((), ())), preferred_element_type=jnp.float32)


def outer48(x, y):
    xh, xm, xl = [p.astype(jnp.float32) for p in split3(x)]
    yh, ym, yl = [p.astype(jnp.float32) for p in split3(y)]
    left = jnp.concatenate([xh, xm, xh, xm, xh, xl], axis=0).astype(jnp.bfloat16)
    right = jnp.concatenate([yh, ym, ym, yh, yl, yh], axis=0).astype(jnp.bfloat16)
    return lax.dot_general(left, right, (((0,), (0,)), ((), ())), preferred_element_type=jnp.float32)


def factor_kernel(g_ref, ptop_ref, facet_ref, tau_ref, tau8_ref, rit_ref, uit_ref, u_ref, li_ref, gr_v, bl_v, te_v, r_v, lt_v):
    nt = NC // 8
    lane = lax.broadcasted_iota(jnp.int32, (8, NC), 1)
    sub = lax.broadcasted_iota(jnp.int32, (8, NC), 0)
    rows = lax.broadcasted_iota(jnp.int32, (NC, NC), 0)
    cols = lax.broadcasted_iota(jnp.int32, (NC, NC), 1)
    eye = jnp.where(rows == cols, 1.0, 0.0)

    def row_of(tile, s):
        return jnp.broadcast_to(tile[s:s + 1, :], (8, NC))

    def col_of(tile, k):
        return jnp.broadcast_to(tile[:, k:k + 1], (8, NC))

    gr_v[:, 0:NC] = g_ref[...]
    bl_v[:, 0:NC] = ptop_ref[...].T
    te_v[:, 0:NC] = ptop_ref[...]
    for ref in (gr_v, bl_v, te_v):
        ref[:, NC:2 * NC] = eye
    tau_row = jnp.zeros((8, NC), jnp.float32)
    gr, bl, te = gr_v[0:8, :], bl_v[0:8, :], te_v[0:8, :]
    for block in range(nt):
        o = 8 * block
        gd, rid = gr[:, 0:NC], gr[:, NC:]
        bd, lid = bl[:, 0:NC], bl[:, NC:]
        cg = [col_of(gd, o + s) for s in range(8)]
        cb = [col_of(bd, o + s) for s in range(8)]
        bt = [row_of(te[:, 0:NC], s) for s in range(8)]
        e = [row_of(te[:, NC:], s) for s in range(8)]
        zero = jnp.zeros((8, NC), jnp.float32)
        r_b = ri_b = u_b = li_b = l_b = y_b = neg = zero
        for s in range(8):
            k = o + s
            diag = row_of(cg[s], s)
            rs = lax.rsqrt(diag)
            norm = diag * rs
            alpha = row_of(cb[s], s)
            sgn = jnp.where(alpha >= 0.0, 1.0, -1.0)
            beta = -sgn * norm
            inv = 1.0 / (alpha - beta)
            fg = cg[s] * rs
            fb = cb[s] * inv
            lrow = jnp.where(lane > k, bt[s] * inv, 0.0)
            yrow = e[s] * inv
            for j in range(s + 1, 8):
                rj = row_of(fg, j)
                uj = row_of(cb[j], s) + sgn * rj
                cg[j] = cg[j] - fg * rj
                cb[j] = cb[j] - fb * uj
                bt[j] = bt[j] - lrow * uj
                e[j] = e[j] - yrow * uj
            rrow = jnp.where(lane >= k, row_of(gd, s) * rs, 0.0)
            rirow = row_of(rid, s) * rs
            lirow = row_of(lid, s)
            urow = jnp.where(lane >= k, row_of(bd, s) + sgn * rrow, 0.0)
            gd = gd - fg * rrow
            rid = rid - fg * rirow
            bd = bd - fb * urow
            lid = lid - fb * lirow
            here = sub == s
            r_b = jnp.where(here, rrow, r_b)
            ri_b = jnp.where(here, rirow, ri_b)
            u_b = jnp.where(here, urow, u_b)
            li_b = jnp.where(here, lirow, li_b)
            l_b = jnp.where(here, lrow, l_b)
            y_b = jnp.where(here, yrow, y_b)
            neg = jnp.where(here, -sgn, neg)
            tau_row = jnp.where(lane == k, (beta - alpha) / beta, tau_row)
        tile = slice(o, o + 8)
        r_v[tile, :] = r_b * neg
        rit_ref[tile, :] = ri_b * neg
        u_ref[tile, :] = u_b
        li_ref[tile, :] = li_b
        lt_v[tile, :] = l_b
        uit_ref[tile, :] = y_b
        if block + 1 < nt:
            new = []
            for ref, x, y in ((gr_v, r_b, (r_b, ri_b)), (bl_v, l_b, (u_b, li_b)), (te_v, u_b, (l_b, y_b))):
                prod = outer48(x, jnp.concatenate(y, axis=1))
                new.append(ref[o + 8:o + 16, :] - prod[o + 8:o + 16])
                if block + 2 < nt:
                    ref[o + 16:, :] = ref[o + 16:, :] - prod[o + 16:]
            gr, bl, te = new
    tau_ref[...] = tau_row[0:1]
    tau8_ref[...] = tau_row
    facet_ref[...] = jnp.where(cols > rows, lt_v[...], r_v[...].T)


def finish_kernel(tau8_ref, rit_ref, uit_ref, u_ref, li_ref, tfac_ref, nmat_ref):
    limat = li_ref[...]
    nmat_ref[...] = dot6(limat.T, uit_ref[...], (1, 0))
    tful = -dot6(dot6(u_ref[...], rit_ref[...], (1, 1)), limat, (1, 1))
    rows = lax.broadcasted_iota(jnp.int32, (NC, NC), 0)
    cols = lax.broadcasted_iota(jnp.int32, (NC, NC), 1)
    tful = jnp.where(cols > rows, tful, 0.0)
    tful = jnp.where(cols == rows, jnp.broadcast_to(tau8_ref[0:1, :], (NC, NC)), tful)
    for j in range(PANELS):
        tfac_ref[j] = tful[j * BW:(j + 1) * BW, j * BW:(j + 1) * BW]


def factor(gram, ptop):
    sq = jax.ShapeDtypeStruct((NC, NC), jnp.float32)
    vm = pl.BlockSpec(memory_space=pltpu.VMEM)
    tau = jax.ShapeDtypeStruct((1, NC), jnp.float32)
    return pl.pallas_call(
        factor_kernel,
        out_shape=(sq, tau, jax.ShapeDtypeStruct((8, NC), jnp.float32), sq, sq, sq, sq),
        in_specs=[vm] * 2,
        out_specs=(vm,) * 7,
        scratch_shapes=[pltpu.VMEM((NC, 2 * NC), jnp.float32)] * 3 + [pltpu.VMEM((NC, NC), jnp.float32)] * 2,
        compiler_params=pltpu.CompilerParams(vmem_limit_bytes=8 * 1024 * 1024),
        cost_estimate=pl.CostEstimate(flops=1_000_000_000, bytes_accessed=600_000, transcendentals=0),
        name="factor",
    )(gram, ptop)


def finish(tau8, rit, uit, u, li):
    vm = pl.BlockSpec(memory_space=pltpu.VMEM)
    return pl.pallas_call(
        finish_kernel,
        out_shape=(jax.ShapeDtypeStruct((PANELS, BW, BW), jnp.float32), jax.ShapeDtypeStruct((NC, NC), jnp.float32)),
        in_specs=[vm] * 5,
        out_specs=(vm,) * 2,
        compiler_params=pltpu.CompilerParams(vmem_limit_bytes=4 * 1024 * 1024),
        cost_estimate=pl.CostEstimate(flops=300_000_000, bytes_accessed=400_000, transcendentals=0),
        name="finish",
    )(tau8, rit, uit, u, li)


def gather_kernel(at_ref, a_v, pt_out, xh_out, xo_out, g_out, ptop_out, head_out,
                  pt_v, x_v, g_v, g_in, x_in, head_v, ptop_v,
                  a_sem, own_sem, send, fwd, recv, h_sem, hsend, hrecv, psend, precv, gsend, grecv, xsend, xrecv):
    ncol, local_rows = at_ref.shape
    nch = local_rows // CH
    half = ncol // 2
    q = lax.axis_index('col')
    r = lax.axis_index('row')
    last = lax.axis_size('col') - 1

    def own_load(c):
        return pltpu.make_async_copy(at_ref.at[pl.ds(0, BW), pl.ds(c * CH, CH)], pt_v.at[c, q], own_sem.at[c])

    def a_load(c):
        return pltpu.make_async_copy(at_ref.at[:, pl.ds(c * CH, CH)], a_v.at[c], a_sem.at[c])

    def hop(c, j, to, sem):
        return pltpu.make_async_remote_copy(
            src_ref=pt_v.at[c, j], dst_ref=pt_v.at[c, j], send_sem=sem, recv_sem=recv.at[c, j],
            device_id={'col': to}, device_id_type=MESH)

    at_end = jnp.logical_or(q == 0, q == last)
    inward = jnp.where(q == 0, 1, -1)
    routes = ((q + 2 * inward, at_end, 0), (q + inward, at_end, 1), (q + 1, jnp.logical_not(at_end), 0), (q - 1, jnp.logical_not(at_end), 1))

    def send_own(c):
        own_load(c).wait()
        for to, valid, slot in routes:
            @pl.when(valid)
            def _():
                hop(c, q, to, send.at[c, slot]).start()

    def head_send(p):
        return pltpu.make_async_remote_copy(
            src_ref=at_ref.at[:, pl.ds(0, NC)], dst_ref=head_v, send_sem=hsend.at[p], recv_sem=hrecv,
            device_id={'row': p}, device_id_type=MESH)

    def ptop_send(p):
        return pltpu.make_async_remote_copy(
            src_ref=pt_v.at[0, :, :, pl.ds(0, NC)], dst_ref=ptop_v, send_sem=psend.at[p], recv_sem=precv,
            device_id={'row': p}, device_id_type=MESH)

    for c in range(nch):
        own_load(c).start()
    for c in range(nch):
        a_load(c).start()

    barrier = pltpu.get_barrier_semaphore()

    for to, valid in ((q + 2, q + 2 <= last), (q - 2, q >= 2), (q + 1, q < last), (q - 1, q > 0)):
        @pl.when(valid)
        def _():
            pl.semaphore_signal(barrier, inc=1, device_id={'col': to}, device_id_type=MESH)

    for d in range(1, 4):
        pl.semaphore_signal(barrier, inc=1, device_id={'row': (r + d) % 4}, device_id_type=MESH)
    inner = jnp.logical_not(at_end)
    outward = jnp.where(q == 1, -1, 1)

    @pl.when(inner)
    def _():
        pl.semaphore_wait(barrier, 6)

    @pl.when(jnp.logical_not(inner))
    def _():
        pl.semaphore_wait(barrier, 5)

    for c in range(nch):
        send_own(c)

    head_local = pltpu.make_async_copy(at_ref.at[:, pl.ds(0, NC)], head_v, h_sem)

    @pl.when(r == 0)
    def _():
        for p in range(1, 4):
            head_send(p).start()
        head_local.start()

    x_v[...] = jnp.zeros_like(x_v)
    g_v[...] = jnp.zeros_like(g_v)

    g_copies = []
    for d in range(1, 4):
        g_copies.append(pltpu.make_async_remote_copy(
            src_ref=g_v, dst_ref=g_in.at[d - 1], send_sem=gsend.at[d - 1], recv_sem=grecv.at[d - 1],
            device_id={'row': (r + d) % 4}, device_id_type=MESH))

    def chunk(c, carry):
        near, far = q - outward, q - 2 * outward

        @pl.when(inner)
        def _():
            hop(c, near, q, fwd.at[c, 0]).wait_recv()
            hop(c, near, q + outward, fwd.at[c, 0]).start()
            hop(c, far, q, fwd.at[c, 1]).wait_recv()
            hop(c, far, q + outward, fwd.at[c, 1]).start()
            hop(c, q + outward, q, fwd.at[c, 0]).wait_recv()

        @pl.when(at_end)
        def _():
            for d in range(1, 4):
                hop(c, q + d * inward, q, fwd.at[c, 0]).wait_recv()

        pt_out[c] = pt_v[c]

        @pl.when(jnp.logical_and(c == 0, r == 0))
        def _():
            for p in range(1, 4):
                ptop_send(p).start()
            for j in range(PANELS):
                ptop_out[j * BW:(j + 1) * BW, :] = pt_v[0, j, :, 0:NC]

        a_load(c).wait()
        p = pt_v[c].reshape(NC, CH)
        g_v[...] += dot_nt(p, p)

        @pl.when(c == nch - 1)
        def _():
            for g_copy in g_copies:
                g_copy.start()

        x_v[...] += dot_nt(a_v[c], p)
        return carry

    lax.fori_loop(0, nch, chunk, 0)

    core = r % 2
    mate = r + 1 - 2 * core
    x_copy = pltpu.make_async_remote_copy(
        src_ref=x_v, dst_ref=x_in, send_sem=xsend, recv_sem=xrecv,
        device_id={'row': mate}, device_id_type=MESH)
    x_copy.start()
    @pl.when(r == 0)
    def _():
        for p in range(1, 4):
            head_send(p).wait_send()
            ptop_send(p).wait_send()
        head_local.wait()

    @pl.when(r > 0)
    def _():
        head_send(0).wait_recv()
        ptop_send(0).wait_recv()
        for j in range(PANELS):
            ptop_out[j * BW:(j + 1) * BW, :] = ptop_v[j]

    head_out[...] = head_v[...]

    def drain(c, carry):
        for to, valid, slot in routes:
            @pl.when(valid)
            def _():
                hop(c, q, to, send.at[c, slot]).wait_send()

        @pl.when(inner)
        def _():
            for slot in range(2):
                hop(c, q, q, fwd.at[c, slot]).wait_send()

        return carry

    lax.fori_loop(0, nch, drain, 0)
    for g_copy in g_copies:
        g_copy.wait()
    parts = [g_v[...]] + [g_in[d - 1] for d in range(1, 4)]
    total = None
    for row in range(4):
        dist = (r - row + 4) % 4
        part = jnp.where(dist == 0, parts[0], jnp.where(dist == 1, parts[1], jnp.where(dist == 2, parts[2], parts[3])))
        total = part if total is None else total + part
    g_out[...] = total
    x_copy.wait()
    mine, other = pl.ds(half * core, half), pl.ds(half * (1 - core), half)
    xh_out[...] = x_v[mine, :] + x_in[mine, :]
    xo_out[...] = x_v[other, :] + x_in[other, :]


def gather(at):
    ncol, local_rows = at.shape
    nch = local_rows // CH
    f32 = jnp.float32
    vm, anys = pl.BlockSpec(memory_space=pltpu.VMEM), pl.BlockSpec(memory_space=pl.ANY)
    dma = pltpu.SemaphoreType.DMA
    return pl.pallas_call(
        gather_kernel,
        out_shape=(jax.ShapeDtypeStruct((nch, ncol, CH), f32), jax.ShapeDtypeStruct((nch, PANELS, BW, CH), f32), jax.ShapeDtypeStruct((ncol // 2, NC), f32), jax.ShapeDtypeStruct((ncol // 2, NC), f32),
                   jax.ShapeDtypeStruct((NC, NC), f32), jax.ShapeDtypeStruct((NC, NC), f32), jax.ShapeDtypeStruct((ncol, NC), f32)),
        in_specs=[anys],
        out_specs=(vm,) * 7,
        scratch_shapes=[pltpu.VMEM((nch, PANELS, BW, CH), f32), pltpu.VMEM((ncol, NC), f32),
                        pltpu.VMEM((NC, NC), f32), pltpu.VMEM((3, NC, NC), f32), pltpu.VMEM((ncol, NC), f32),
                        pltpu.VMEM((ncol, NC), f32), pltpu.VMEM((PANELS, BW, NC), f32),
                        dma((nch,)), dma((nch,)), dma((nch, 2)), dma((nch, 2)), dma((nch, 4)), dma, dma((4,)), dma, dma((4,)), dma,
                        dma((3,)), dma((3,)), dma, dma],
        compiler_params=pltpu.CompilerParams(collective_id=0, has_side_effects=True, vmem_limit_bytes=GATHER_VMEM),
        name="gather",
    )(at)


def update_kernel(a_ref, pt_ref, x0_ref, x1_ref, x2_ref, x3_ref, head_ref, rit_ref, nmat_ref, uit_ref, facet_ref, out_ref, z_v, top_v, sem, *strips):
    q = lax.axis_index('col')
    r = lax.axis_index('row')
    ncol = head_ref.shape[0]
    half = ncol // 2
    core = r % 2
    rit = rit_ref[...]
    nmat = nmat_ref[...]
    mine = pl.multiple_of(half * core, half)
    other = pl.multiple_of(half * (1 - core), half)
    for lo, xa, xb in ((mine, x0_ref, x1_ref), (other, x2_ref, x3_ref)):
        r12t = dot6(xa[...] + xb[...], rit, (1, 1))
        top_v[pl.ds(lo, half), :] = r12t
        z_v[pl.ds(lo, half), :] = stack6(dot6(head_ref[pl.ds(lo, half), :] - r12t, nmat, (1, 0)), 1, LEFT)
    own = pl.ds(pl.multiple_of(q * BW, BW), BW)
    top_v[0:BW, :] = facet_ref[own, :]
    z_v[0:BW, :] = stack6(-uit_ref[own, :], 1, LEFT)

    copies = []
    for step, strip in enumerate(strips):
        wide = stack6(pt_ref[step].reshape(NC, CH), 0, RIGHT)
        parts = 2 if step == len(strips) - 1 else 1
        size = ncol // parts
        for part in range(parts):
            lo = part * size
            prod = lax.dot_general(z_v[lo:lo + size, :], wide, (((1,), (0,)), ((), ())), preferred_element_type=jnp.float32)
            if part == 0:
                new = jnp.concatenate([-prod[0:BW], a_ref[step, BW:size, :] - prod[BW:]], axis=0)
            else:
                new = a_ref[step, lo:lo + size, :] - prod
            if step == 0:
                strip[:, 0:NC] = jnp.where(r == 0, top_v[...], new[:, 0:NC])
                strip[:, NC:] = new[:, NC:]
            else:
                strip[lo:lo + size, :] = new
            copies.append(pltpu.make_async_copy(
                strip.at[pl.ds(lo, size)], out_ref.at[pl.ds(lo, size), pl.ds(step * CH, CH)], sem.at[len(copies)]))
            copies[-1].start()
    for copy in copies:
        copy.wait()


def update(a, pt, xs, head, rit, nmat, uit, facet):
    nch, ncol, _ = a.shape
    vm = pl.BlockSpec(memory_space=pltpu.VMEM)
    return pl.pallas_call(
        update_kernel,
        out_shape=jax.ShapeDtypeStruct((ncol, nch * CH), jnp.float32),
        in_specs=[vm] * 11,
        out_specs=pl.BlockSpec(memory_space=pl.ANY),
        scratch_shapes=[pltpu.VMEM((ncol, 6 * NC), jnp.bfloat16), pltpu.VMEM((ncol, NC), jnp.float32), pltpu.SemaphoreType.DMA((nch + 1,))]
        + [pltpu.VMEM((ncol, CH), jnp.float32)] * nch,
        compiler_params=pltpu.CompilerParams(vmem_limit_bytes=UPDATE_VMEM),
        name="update",
    )(a, pt, *xs, head, rit, nmat, uit, facet)


def solution(mesh):
    block_spec = P(('batch', 'row'), 'col', None)

    def device_fn(a_local):
        local_rows, local_blocks, bw = a_local.shape
        ncol = local_blocks * bw
        at = a_local.transpose(1, 2, 0).reshape(ncol, local_rows)
        a, pt, xh, xo, gram, ptop, head = gather(at)
        x1 = lax.ppermute(xh, 'row', [(i, i ^ 2) for i in range(4)])
        facet, tau, tau8, rit, uit, u, li = factor(gram, ptop)
        x1, u = lax.optimization_barrier((x1, u))
        x3 = lax.ppermute(x1, 'row', [(i, i ^ 1) for i in range(4)])
        tfac, nmat = finish(tau8, rit, uit, u, li)
        out = update(a, pt, (xh, x1, xo, x3), head, rit, nmat, uit, facet)
        a_out = out.reshape(local_blocks, bw, local_rows).transpose(2, 0, 1)
        return a_out, tau.reshape(NC), tfac

    return jax.shard_map(device_fn, mesh=mesh, in_specs=(block_spec,), out_specs=(block_spec, P('batch'), P('batch', None, None)), check_vma=False)
```

```python
import functools
import jax
import jax.numpy as jnp
from jax import lax
from jax.experimental import pallas as pl
from jax.experimental.pallas import tpu as pltpu
from jax.sharding import PartitionSpec as P

PANELS = 4
BW = 32
NC = PANELS * BW
CH = 512
UPDATE_VMEM = 32 * 1024 * 1024
GATHER_VMEM = 32 * 1024 * 1024
HIGHEST = lax.Precision.HIGHEST
MESH = pl.DeviceIdType.MESH


def dot_nt(x, y):
    return lax.dot_general(x, y, (((1,), (1,)), ((), ())), precision=HIGHEST, preferred_element_type=jnp.float32)


def dot16_nt(x, y):
    return lax.dot_general(x, y, (((1,), (1,)), ((), ())), preferred_element_type=jnp.float32)


def split3(x):
    hi = x.astype(jnp.bfloat16)
    rem = x - hi.astype(jnp.float32)
    mid = rem.astype(jnp.bfloat16)
    lo = (rem - mid.astype(jnp.float32)).astype(jnp.bfloat16)
    return hi, mid, lo


def stack6(x, axis, order):
    parts = split3(x)
    return jnp.concatenate([parts[i] for i in order], axis=axis)


LEFT, RIGHT = (0, 1, 0, 1, 0, 2), (0, 1, 1, 0, 2, 0)


def dot6(x, y, dims):
    left = stack6(x, dims[0], LEFT)
    right = stack6(y, dims[1], RIGHT)
    return lax.dot_general(left, right, (((dims[0],), (dims[1],)), ((), ())), preferred_element_type=jnp.float32)


def outer48(x, y):
    xh, xm, xl = [p.astype(jnp.float32) for p in split3(x)]
    yh, ym, yl = [p.astype(jnp.float32) for p in split3(y)]
    left = jnp.concatenate([xh, xm, xh, xm, xh, xl], axis=0).astype(jnp.bfloat16)
    right = jnp.concatenate([yh, ym, ym, yh, yl, yh], axis=0).astype(jnp.bfloat16)
    return lax.dot_general(left, right, (((0,), (0,)), ((), ())), preferred_element_type=jnp.float32)


def factor_kernel(g_ref, ptop_ref, facet_ref, tau_ref, tau8_ref, rit_ref, uit_ref, u_ref, li_ref, gr_v, bl_v, te_v, r_v, lt_v):
    nt = NC // 8
    lane = lax.broadcasted_iota(jnp.int32, (8, NC), 1)
    sub = lax.broadcasted_iota(jnp.int32, (8, NC), 0)
    rows = lax.broadcasted_iota(jnp.int32, (NC, NC), 0)
    cols = lax.broadcasted_iota(jnp.int32, (NC, NC), 1)
    eye = jnp.where(rows == cols, 1.0, 0.0)

    def row_of(tile, s):
        return jnp.broadcast_to(tile[s:s + 1, :], (8, NC))

    def col_of(tile, k):
        return jnp.broadcast_to(tile[:, k:k + 1], (8, NC))

    gr_v[:, 0:NC] = g_ref[...]
    bl_v[:, 0:NC] = ptop_ref[...].T
    te_v[:, 0:NC] = ptop_ref[...]
    for ref in (gr_v, bl_v, te_v):
        ref[:, NC:2 * NC] = eye
    tau_row = jnp.zeros((8, NC), jnp.float32)
    gr, bl, te = gr_v[0:8, :], bl_v[0:8, :], te_v[0:8, :]
    for block in range(nt):
        o = 8 * block
        gd, rid = gr[:, 0:NC], gr[:, NC:]
        bd, lid = bl[:, 0:NC], bl[:, NC:]
        cg = [col_of(gd, o + s) for s in range(8)]
        cb = [col_of(bd, o + s) for s in range(8)]
        bt = [row_of(te[:, 0:NC], s) for s in range(8)]
        e = [row_of(te[:, NC:], s) for s in range(8)]
        zero = jnp.zeros((8, NC), jnp.float32)
        r_b = ri_b = u_b = li_b = l_b = y_b = neg = zero
        for s in range(8):
            k = o + s
            diag = row_of(cg[s], s)
            rs = lax.rsqrt(diag)
            norm = diag * rs
            alpha = row_of(cb[s], s)
            sgn = jnp.where(alpha >= 0.0, 1.0, -1.0)
            beta = -sgn * norm
            inv = 1.0 / (alpha - beta)
            fg = cg[s] * rs
            fb = cb[s] * inv
            lrow = jnp.where(lane > k, bt[s] * inv, 0.0)
            yrow = e[s] * inv
            for j in range(s + 1, 8):
                rj = row_of(fg, j)
                uj = row_of(cb[j], s) + sgn * rj
                cg[j] = cg[j] - fg * rj
                cb[j] = cb[j] - fb * uj
                bt[j] = bt[j] - lrow * uj
                e[j] = e[j] - yrow * uj
            rrow = jnp.where(lane >= k, row_of(gd, s) * rs, 0.0)
            rirow = row_of(rid, s) * rs
            lirow = row_of(lid, s)
            urow = jnp.where(lane >= k, row_of(bd, s) + sgn * rrow, 0.0)
            gd = gd - fg * rrow
            rid = rid - fg * rirow
            bd = bd - fb * urow
            lid = lid - fb * lirow
            here = sub == s
            r_b = jnp.where(here, rrow, r_b)
            ri_b = jnp.where(here, rirow, ri_b)
            u_b = jnp.where(here, urow, u_b)
            li_b = jnp.where(here, lirow, li_b)
            l_b = jnp.where(here, lrow, l_b)
            y_b = jnp.where(here, yrow, y_b)
            neg = jnp.where(here, -sgn, neg)
            tau_row = jnp.where(lane == k, (beta - alpha) / beta, tau_row)
        tile = slice(o, o + 8)
        r_v[tile, :] = r_b * neg
        rit_ref[tile, :] = ri_b * neg
        u_ref[tile, :] = u_b
        li_ref[tile, :] = li_b
        lt_v[tile, :] = l_b
        uit_ref[tile, :] = y_b
        if block + 1 < nt:
            new = []
            for ref, x, y in ((gr_v, r_b, (r_b, ri_b)), (bl_v, l_b, (u_b, li_b)), (te_v, u_b, (l_b, y_b))):
                prod = outer48(x, jnp.concatenate(y, axis=1))
                new.append(ref[o + 8:o + 16, :] - prod[o + 8:o + 16])
                if block + 2 < nt:
                    ref[o + 16:, :] = ref[o + 16:, :] - prod[o + 16:]
            gr, bl, te = new
    tau_ref[...] = tau_row[0:1]
    tau8_ref[...] = tau_row
    facet_ref[...] = jnp.where(cols > rows, lt_v[...], r_v[...].T)


def finish_kernel(tau8_ref, rit_ref, uit_ref, u_ref, li_ref, tfac_ref, nmat_ref):
    limat = li_ref[...]
    nmat_ref[...] = dot6(limat.T, uit_ref[...], (1, 0))
    tful = -dot6(dot6(u_ref[...], rit_ref[...], (1, 1)), limat, (1, 1))
    rows = lax.broadcasted_iota(jnp.int32, (NC, NC), 0)
    cols = lax.broadcasted_iota(jnp.int32, (NC, NC), 1)
    tful = jnp.where(cols > rows, tful, 0.0)
    tful = jnp.where(cols == rows, jnp.broadcast_to(tau8_ref[0:1, :], (NC, NC)), tful)
    for j in range(PANELS):
        tfac_ref[j] = tful[j * BW:(j + 1) * BW, j * BW:(j + 1) * BW]


def factor(gram, ptop):
    sq = jax.ShapeDtypeStruct((NC, NC), jnp.float32)
    vm = pl.BlockSpec(memory_space=pltpu.VMEM)
    tau = jax.ShapeDtypeStruct((1, NC), jnp.float32)
    return pl.pallas_call(
        factor_kernel,
        out_shape=(sq, tau, jax.ShapeDtypeStruct((8, NC), jnp.float32), sq, sq, sq, sq),
        in_specs=[vm] * 2,
        out_specs=(vm,) * 7,
        scratch_shapes=[pltpu.VMEM((NC, 2 * NC), jnp.float32)] * 3 + [pltpu.VMEM((NC, NC), jnp.float32)] * 2,
        compiler_params=pltpu.CompilerParams(vmem_limit_bytes=8 * 1024 * 1024),
        cost_estimate=pl.CostEstimate(flops=1_000_000_000, bytes_accessed=600_000, transcendentals=0),
        name="factor",
    )(gram, ptop)


def finish(tau8, rit, uit, u, li):
    vm = pl.BlockSpec(memory_space=pltpu.VMEM)
    return pl.pallas_call(
        finish_kernel,
        out_shape=(jax.ShapeDtypeStruct((PANELS, BW, BW), jnp.float32), jax.ShapeDtypeStruct((NC, NC), jnp.float32)),
        in_specs=[vm] * 5,
        out_specs=(vm,) * 2,
        compiler_params=pltpu.CompilerParams(vmem_limit_bytes=4 * 1024 * 1024),
        cost_estimate=pl.CostEstimate(flops=300_000_000, bytes_accessed=400_000, transcendentals=0),
        name="finish",
    )(tau8, rit, uit, u, li)


def gather_kernel(at_ref, a_v, pt_out, xh_out, xo_out, g_out, ptop_out, head_out,
                  pt_v, x_v, g_v, g_in, g_sum, g_end, x_in, head_v, ptop_v,
                  a_sem, own_sem, send, fwd, recv, h_sem, hsend, hrecv, psend, precv, gsend, grecv, xsend, xrecv):
    ncol, local_rows = at_ref.shape
    nch = local_rows // CH
    half = ncol // 2
    q = lax.axis_index('col')
    r = lax.axis_index('row')
    last = lax.axis_size('col') - 1

    def own_load(c):
        return pltpu.make_async_copy(at_ref.at[pl.ds(0, BW), pl.ds(c * CH, CH)], pt_v.at[c, q], own_sem.at[c])

    def a_load(c):
        return pltpu.make_async_copy(at_ref.at[:, pl.ds(c * CH, CH)], a_v.at[c], a_sem.at[c])

    def hop(c, j, to, sem):
        return pltpu.make_async_remote_copy(
            src_ref=pt_v.at[c, j], dst_ref=pt_v.at[c, j], send_sem=sem, recv_sem=recv.at[c, j],
            device_id={'col': to}, device_id_type=MESH)

    at_end = jnp.logical_or(q == 0, q == last)
    inward = jnp.where(q == 0, 1, -1)
    routes = ((q + 2 * inward, at_end, 0), (q + inward, at_end, 1), (q + 1, jnp.logical_not(at_end), 0), (q - 1, jnp.logical_not(at_end), 1))

    def send_own(c):
        own_load(c).wait()
        for to, valid, slot in routes:
            @pl.when(valid)
            def _():
                hop(c, q, to, send.at[c, slot]).start()

    def head_send(p):
        return pltpu.make_async_remote_copy(
            src_ref=at_ref.at[:, pl.ds(0, NC)], dst_ref=head_v, send_sem=hsend.at[p], recv_sem=hrecv,
            device_id={'row': p}, device_id_type=MESH)

    def ptop_send(p):
        return pltpu.make_async_remote_copy(
            src_ref=pt_v.at[0, :, :, pl.ds(0, NC)], dst_ref=ptop_v, send_sem=psend.at[p], recv_sem=precv,
            device_id={'row': p}, device_id_type=MESH)

    for c in range(nch):
        own_load(c).start()
    for c in range(nch):
        a_load(c).start()

    barrier = pltpu.get_barrier_semaphore()

    for to, valid in ((q + 2, q + 2 <= last), (q - 2, q >= 2), (q + 1, q < last), (q - 1, q > 0)):
        @pl.when(valid)
        def _():
            pl.semaphore_signal(barrier, inc=1, device_id={'col': to}, device_id_type=MESH)

    for d in range(1, 4):
        pl.semaphore_signal(barrier, inc=1, device_id={'row': (r + d) % 4}, device_id_type=MESH)
    inner = jnp.logical_not(at_end)
    outward = jnp.where(q == 1, -1, 1)

    @pl.when(inner)
    def _():
        pl.semaphore_wait(barrier, 6)

    @pl.when(jnp.logical_not(inner))
    def _():
        pl.semaphore_wait(barrier, 5)

    for c in range(nch):
        send_own(c)

    head_local = pltpu.make_async_copy(at_ref.at[:, pl.ds(0, NC)], head_v, h_sem)

    @pl.when(r == 0)
    def _():
        for p in range(1, 4):
            head_send(p).start()
        head_local.start()

    x_v[...] = jnp.zeros_like(x_v)
    g_v[...] = jnp.zeros_like(g_v)

    g_copies = []
    for d in range(1, 4):
        g_copies.append(pltpu.make_async_remote_copy(
            src_ref=g_v, dst_ref=g_in.at[d - 1], send_sem=gsend.at[d - 1], recv_sem=grecv.at[d - 1],
            device_id={'row': (r + d) % 4}, device_id_type=MESH))

    def chunk(c, carry):
        near, far = q - outward, q - 2 * outward

        @pl.when(inner)
        def _():
            hop(c, near, q, fwd.at[c, 0]).wait_recv()
            hop(c, near, q + outward, fwd.at[c, 0]).start()
            hop(c, far, q, fwd.at[c, 1]).wait_recv()
            hop(c, far, q + outward, fwd.at[c, 1]).start()
            hop(c, q + outward, q, fwd.at[c, 0]).wait_recv()

        @pl.when(at_end)
        def _():
            for d in range(1, 4):
                hop(c, q + d * inward, q, fwd.at[c, 0]).wait_recv()

        pt_out[c] = pt_v[c]

        @pl.when(jnp.logical_and(c == 0, r == 0))
        def _():
            for p in range(1, 4):
                ptop_send(p).start()
            for j in range(PANELS):
                ptop_out[j * BW:(j + 1) * BW, :] = pt_v[0, j, :, 0:NC]

        a_load(c).wait()
        p = pt_v[c].reshape(NC, CH)
        @pl.when(inner)
        def _():
            g_v[...] += dot_nt(p, p)

        @pl.when(jnp.logical_and(c == nch - 1, inner))
        def _():
            for g_copy in g_copies:
                g_copy.start()

        ah, am, al = split3(a_v[c])
        ph, pm, plo = split3(p)
        both = jnp.concatenate([ph, pm], axis=0)
        main = dot16_nt(ah, both) + dot16_nt(am, both)
        low = dot16_nt(jnp.concatenate([ah, al], axis=1), jnp.concatenate([plo, ph], axis=1))
        x_v[...] += main[:, 0:NC] + (main[:, NC:] + low)
        return carry

    lax.fori_loop(0, nch, chunk, 0)

    core = r % 2
    mate = r + 1 - 2 * core
    x_copy = pltpu.make_async_remote_copy(
        src_ref=x_v, dst_ref=x_in, send_sem=xsend, recv_sem=xrecv,
        device_id={'row': mate}, device_id_type=MESH)
    x_copy.start()

    part = pl.ds((NC // 2) * core, NC // 2)

    def half_copy(to):
        return pltpu.make_async_remote_copy(
            src_ref=g_sum.at[part], dst_ref=g_end.at[part], send_sem=gsend.at[3], recv_sem=grecv.at[3],
            device_id={'col': to}, device_id_type=MESH)

    mate_copy = pltpu.make_async_remote_copy(
        src_ref=g_end.at[part], dst_ref=g_end.at[part], send_sem=gsend.at[4], recv_sem=grecv.at[4],
        device_id={'row': mate}, device_id_type=MESH)
    @pl.when(r == 0)
    def _():
        for p in range(1, 4):
            head_send(p).wait_send()
            ptop_send(p).wait_send()
        head_local.wait()

    @pl.when(r > 0)
    def _():
        head_send(0).wait_recv()
        ptop_send(0).wait_recv()
        for j in range(PANELS):
            ptop_out[j * BW:(j + 1) * BW, :] = ptop_v[j]

    head_out[...] = head_v[...]

    def drain(c, carry):
        for to, valid, slot in routes:
            @pl.when(valid)
            def _():
                hop(c, q, to, send.at[c, slot]).wait_send()

        @pl.when(inner)
        def _():
            for slot in range(2):
                hop(c, q, q, fwd.at[c, slot]).wait_send()

        return carry

    lax.fori_loop(0, nch, drain, 0)
    @pl.when(inner)
    def _():
        for g_copy in g_copies:
            g_copy.wait()
        parts = [g_v[...]] + [g_in[d - 1] for d in range(1, 4)]
        total = None
        for row in range(4):
            dist = (r - row + 4) % 4
            part = jnp.where(dist == 0, parts[0], jnp.where(dist == 1, parts[1], jnp.where(dist == 2, parts[2], parts[3])))
            total = part if total is None else total + part
        g_out[...] = total
        g_sum[...] = total

    @pl.when(at_end)
    def _():
        half_copy(q).wait_recv()
        mate_copy.start()

    x_copy.wait()
    mine, other = pl.ds(half * core, half), pl.ds(half * (1 - core), half)
    xh_out[...] = x_v[mine, :] + x_in[mine, :]
    xo_out[...] = x_v[other, :] + x_in[other, :]

    @pl.when(inner)
    def _():
        half_copy(q + outward).start()
        half_copy(q + outward).wait_send()

    @pl.when(at_end)
    def _():
        mate_copy.wait()
        g_out[...] = g_end[...]


def gather(at):
    ncol, local_rows = at.shape
    nch = local_rows // CH
    f32 = jnp.float32
    vm, anys = pl.BlockSpec(memory_space=pltpu.VMEM), pl.BlockSpec(memory_space=pl.ANY)
    dma = pltpu.SemaphoreType.DMA
    return pl.pallas_call(
        gather_kernel,
        out_shape=(jax.ShapeDtypeStruct((nch, ncol, CH), f32), jax.ShapeDtypeStruct((nch, PANELS, BW, CH), f32), jax.ShapeDtypeStruct((ncol // 2, NC), f32), jax.ShapeDtypeStruct((ncol // 2, NC), f32),
                   jax.ShapeDtypeStruct((NC, NC), f32), jax.ShapeDtypeStruct((NC, NC), f32), jax.ShapeDtypeStruct((ncol, NC), f32)),
        in_specs=[anys],
        out_specs=(vm,) * 7,
        scratch_shapes=[pltpu.VMEM((nch, PANELS, BW, CH), f32), pltpu.VMEM((ncol, NC), f32),
                        pltpu.VMEM((NC, NC), f32), pltpu.VMEM((3, NC, NC), f32), pltpu.VMEM((NC, NC), f32), pltpu.VMEM((NC, NC), f32), pltpu.VMEM((ncol, NC), f32),
                        pltpu.VMEM((ncol, NC), f32), pltpu.VMEM((PANELS, BW, NC), f32),
                        dma((nch,)), dma((nch,)), dma((nch, 2)), dma((nch, 2)), dma((nch, 4)), dma, dma((4,)), dma, dma((4,)), dma,
                        dma((5,)), dma((5,)), dma, dma],
        compiler_params=pltpu.CompilerParams(collective_id=0, has_side_effects=True, vmem_limit_bytes=GATHER_VMEM),
        name="gather",
    )(at)


def update_kernel(a_ref, pt_ref, x0_ref, x1_ref, x2_ref, x3_ref, head_ref, rit_ref, nmat_ref, uit_ref, facet_ref, out_ref, z_v, top_v, sem, *strips):
    q = lax.axis_index('col')
    r = lax.axis_index('row')
    ncol = head_ref.shape[0]
    half = ncol // 2
    core = r % 2
    rit = rit_ref[...]
    nmat = nmat_ref[...]
    mine = pl.multiple_of(half * core, half)
    other = pl.multiple_of(half * (1 - core), half)
    for lo, xa, xb in ((mine, x0_ref, x1_ref), (other, x2_ref, x3_ref)):
        r12t = dot6(xa[...] + xb[...], rit, (1, 1))
        top_v[pl.ds(lo, half), :] = r12t
        z_v[pl.ds(lo, half), :] = stack6(dot6(head_ref[pl.ds(lo, half), :] - r12t, nmat, (1, 0)), 1, LEFT)
    own = pl.ds(pl.multiple_of(q * BW, BW), BW)
    top_v[0:BW, :] = facet_ref[own, :]
    z_v[0:BW, :] = stack6(-uit_ref[own, :], 1, LEFT)

    copies = []
    for step, strip in enumerate(strips):
        wide = stack6(pt_ref[step].reshape(NC, CH), 0, RIGHT)
        parts = 2 if step == len(strips) - 1 else 1
        size = ncol // parts
        for part in range(parts):
            lo = part * size
            prod = lax.dot_general(z_v[lo:lo + size, :], wide, (((1,), (0,)), ((), ())), preferred_element_type=jnp.float32)
            if part == 0:
                new = jnp.concatenate([-prod[0:BW], a_ref[step, BW:size, :] - prod[BW:]], axis=0)
            else:
                new = a_ref[step, lo:lo + size, :] - prod
            if step == 0:
                strip[:, 0:NC] = jnp.where(r == 0, top_v[...], new[:, 0:NC])
                strip[:, NC:] = new[:, NC:]
            else:
                strip[lo:lo + size, :] = new
            copies.append(pltpu.make_async_copy(
                strip.at[pl.ds(lo, size)], out_ref.at[pl.ds(lo, size), pl.ds(step * CH, CH)], sem.at[len(copies)]))
            copies[-1].start()
    for copy in copies:
        copy.wait()


def update(a, pt, xs, head, rit, nmat, uit, facet):
    nch, ncol, _ = a.shape
    vm = pl.BlockSpec(memory_space=pltpu.VMEM)
    return pl.pallas_call(
        update_kernel,
        out_shape=jax.ShapeDtypeStruct((ncol, nch * CH), jnp.float32),
        in_specs=[vm] * 11,
        out_specs=pl.BlockSpec(memory_space=pl.ANY),
        scratch_shapes=[pltpu.VMEM((ncol, 6 * NC), jnp.bfloat16), pltpu.VMEM((ncol, NC), jnp.float32), pltpu.SemaphoreType.DMA((nch + 1,))]
        + [pltpu.VMEM((ncol, CH), jnp.float32)] * nch,
        compiler_params=pltpu.CompilerParams(vmem_limit_bytes=UPDATE_VMEM),
        name="update",
    )(a, pt, *xs, head, rit, nmat, uit, facet)


def solution(mesh):
    block_spec = P(('batch', 'row'), 'col', None)

    def device_fn(a_local):
        local_rows, local_blocks, bw = a_local.shape
        ncol = local_blocks * bw
        at = a_local.transpose(1, 2, 0).reshape(ncol, local_rows)
        a, pt, xh, xo, gram, ptop, head = gather(at)
        x1 = lax.ppermute(xh, 'row', [(i, i ^ 2) for i in range(4)])
        facet, tau, tau8, rit, uit, u, li = factor(gram, ptop)
        x1, u = lax.optimization_barrier((x1, u))
        x3 = lax.ppermute(x1, 'row', [(i, i ^ 1) for i in range(4)])
        tfac, nmat = finish(tau8, rit, uit, u, li)
        out = update(a, pt, (xh, x1, xo, x3), head, rit, nmat, uit, facet)
        a_out = out.reshape(local_blocks, bw, local_rows).transpose(2, 0, 1)
        return a_out, tau.reshape(NC), tfac

    return jax.shard_map(device_fn, mesh=mesh, in_specs=(block_spec,), out_specs=(block_spec, P('batch'), P('batch', None, None)), check_vma=False)
```

```python
import functools
import jax
import jax.numpy as jnp
from jax import lax
from jax.experimental import pallas as pl
from jax.experimental.pallas import tpu as pltpu
from jax.sharding import PartitionSpec as P

PANELS = 4
BW = 32
NC = PANELS * BW
CH = 512
UPDATE_VMEM = 32 * 1024 * 1024
WIDE = 2
GATHER_VMEM = 32 * 1024 * 1024
HIGHEST = lax.Precision.HIGHEST
MESH = pl.DeviceIdType.MESH


def dot_nt(x, y):
    return lax.dot_general(x, y, (((1,), (1,)), ((), ())), precision=HIGHEST, preferred_element_type=jnp.float32)


def dot16_nt(x, y):
    return lax.dot_general(x, y, (((1,), (1,)), ((), ())), preferred_element_type=jnp.float32)


def split3(x):
    hi = x.astype(jnp.bfloat16)
    rem = x - hi.astype(jnp.float32)
    mid = rem.astype(jnp.bfloat16)
    lo = (rem - mid.astype(jnp.float32)).astype(jnp.bfloat16)
    return hi, mid, lo


def stack6(x, axis, order):
    parts = split3(x)
    return jnp.concatenate([parts[i] for i in order], axis=axis)


LEFT, RIGHT = (0, 1, 0, 1, 0, 2), (0, 1, 1, 0, 2, 0)


def dot6(x, y, dims):
    left = stack6(x, dims[0], LEFT)
    right = stack6(y, dims[1], RIGHT)
    return lax.dot_general(left, right, (((dims[0],), (dims[1],)), ((), ())), preferred_element_type=jnp.float32)


def outer48(x, y):
    xh, xm, xl = [p.astype(jnp.float32) for p in split3(x)]
    yh, ym, yl = [p.astype(jnp.float32) for p in split3(y)]
    left = jnp.concatenate([xh, xm, xh, xm, xh, xl], axis=0).astype(jnp.bfloat16)
    right = jnp.concatenate([yh, ym, ym, yh, yl, yh], axis=0).astype(jnp.bfloat16)
    return lax.dot_general(left, right, (((0,), (0,)), ((), ())), preferred_element_type=jnp.float32)


def factor_kernel(g_ref, ptop_ref, facet_ref, tau_ref, tau8_ref, rit_ref, uit_ref, u_ref, li_ref, gr_v, bl_v, te_v, r_v, lt_v):
    nt = NC // 8
    lane = lax.broadcasted_iota(jnp.int32, (8, NC), 1)
    sub = lax.broadcasted_iota(jnp.int32, (8, NC), 0)
    rows = lax.broadcasted_iota(jnp.int32, (NC, NC), 0)
    cols = lax.broadcasted_iota(jnp.int32, (NC, NC), 1)
    eye = jnp.where(rows == cols, 1.0, 0.0)

    def row_of(tile, s):
        return jnp.broadcast_to(tile[s:s + 1, :], (8, NC))

    def col_of(tile, k):
        return jnp.broadcast_to(tile[:, k:k + 1], (8, NC))

    gr_v[:, 0:NC] = g_ref[...]
    bl_v[:, 0:NC] = ptop_ref[...].T
    te_v[:, 0:NC] = ptop_ref[...]
    for ref in (gr_v, bl_v, te_v):
        ref[:, NC:2 * NC] = eye
    tau_row = jnp.zeros((8, NC), jnp.float32)
    gr, bl, te = gr_v[0:8, :], bl_v[0:8, :], te_v[0:8, :]
    for block in range(nt):
        o = 8 * block
        gd, rid = gr[:, 0:NC], gr[:, NC:]
        bd, lid = bl[:, 0:NC], bl[:, NC:]
        cg = [col_of(gd, o + s) for s in range(8)]
        cb = [col_of(bd, o + s) for s in range(8)]
        bt = [row_of(te[:, 0:NC], s) for s in range(8)]
        e = [row_of(te[:, NC:], s) for s in range(8)]
        zero = jnp.zeros((8, NC), jnp.float32)
        r_b = ri_b = u_b = li_b = l_b = y_b = neg = zero
        for s in range(8):
            k = o + s
            diag = row_of(cg[s], s)
            rs = lax.rsqrt(diag)
            norm = diag * rs
            alpha = row_of(cb[s], s)
            sgn = jnp.where(alpha >= 0.0, 1.0, -1.0)
            beta = -sgn * norm
            inv = 1.0 / (alpha - beta)
            fg = cg[s] * rs
            fb = cb[s] * inv
            lrow = jnp.where(lane > k, bt[s] * inv, 0.0)
            yrow = e[s] * inv
            for j in range(s + 1, 8):
                rj = row_of(fg, j)
                uj = row_of(cb[j], s) + sgn * rj
                cg[j] = cg[j] - fg * rj
                cb[j] = cb[j] - fb * uj
                bt[j] = bt[j] - lrow * uj
                e[j] = e[j] - yrow * uj
            rrow = jnp.where(lane >= k, row_of(gd, s) * rs, 0.0)
            rirow = row_of(rid, s) * rs
            lirow = row_of(lid, s)
            urow = jnp.where(lane >= k, row_of(bd, s) + sgn * rrow, 0.0)
            gd = gd - fg * rrow
            rid = rid - fg * rirow
            bd = bd - fb * urow
            lid = lid - fb * lirow
            here = sub == s
            r_b = jnp.where(here, rrow, r_b)
            ri_b = jnp.where(here, rirow, ri_b)
            u_b = jnp.where(here, urow, u_b)
            li_b = jnp.where(here, lirow, li_b)
            l_b = jnp.where(here, lrow, l_b)
            y_b = jnp.where(here, yrow, y_b)
            neg = jnp.where(here, -sgn, neg)
            tau_row = jnp.where(lane == k, (beta - alpha) / beta, tau_row)
        tile = slice(o, o + 8)
        r_v[tile, :] = r_b * neg
        rit_ref[tile, :] = ri_b * neg
        u_ref[tile, :] = u_b
        li_ref[tile, :] = li_b
        lt_v[tile, :] = l_b
        uit_ref[tile, :] = y_b
        if block + 1 < nt:
            new = []
            for ref, x, y in ((gr_v, r_b, (r_b, ri_b)), (bl_v, l_b, (u_b, li_b)), (te_v, u_b, (l_b, y_b))):
                prod = outer48(x, jnp.concatenate(y, axis=1))
                new.append(ref[o + 8:o + 16, :] - prod[o + 8:o + 16])
                if block + 2 < nt:
                    ref[o + 16:, :] = ref[o + 16:, :] - prod[o + 16:]
            gr, bl, te = new
    tau_ref[...] = tau_row[0:1]
    tau8_ref[...] = tau_row
    facet_ref[...] = jnp.where(cols > rows, lt_v[...], r_v[...].T)


def finish_kernel(tau8_ref, rit_ref, uit_ref, u_ref, li_ref, tfac_ref, nmat_ref):
    limat = li_ref[...]
    nmat_ref[...] = dot6(limat.T, uit_ref[...], (1, 0))
    tful = -dot6(dot6(u_ref[...], rit_ref[...], (1, 1)), limat, (1, 1))
    rows = lax.broadcasted_iota(jnp.int32, (NC, NC), 0)
    cols = lax.broadcasted_iota(jnp.int32, (NC, NC), 1)
    tful = jnp.where(cols > rows, tful, 0.0)
    tful = jnp.where(cols == rows, jnp.broadcast_to(tau8_ref[0:1, :], (NC, NC)), tful)
    for j in range(PANELS):
        tfac_ref[j] = tful[j * BW:(j + 1) * BW, j * BW:(j + 1) * BW]


def factor(gram, ptop):
    sq = jax.ShapeDtypeStruct((NC, NC), jnp.float32)
    vm = pl.BlockSpec(memory_space=pltpu.VMEM)
    tau = jax.ShapeDtypeStruct((1, NC), jnp.float32)
    return pl.pallas_call(
        factor_kernel,
        out_shape=(sq, tau, jax.ShapeDtypeStruct((8, NC), jnp.float32), sq, sq, sq, sq),
        in_specs=[vm] * 2,
        out_specs=(vm,) * 7,
        scratch_shapes=[pltpu.VMEM((NC, 2 * NC), jnp.float32)] * 3 + [pltpu.VMEM((NC, NC), jnp.float32)] * 2,
        compiler_params=pltpu.CompilerParams(vmem_limit_bytes=8 * 1024 * 1024),
        cost_estimate=pl.CostEstimate(flops=1_000_000_000, bytes_accessed=600_000, transcendentals=0),
        name="factor",
    )(gram, ptop)


def finish(tau8, rit, uit, u, li):
    vm = pl.BlockSpec(memory_space=pltpu.VMEM)
    return pl.pallas_call(
        finish_kernel,
        out_shape=(jax.ShapeDtypeStruct((PANELS, BW, BW), jnp.float32), jax.ShapeDtypeStruct((NC, NC), jnp.float32)),
        in_specs=[vm] * 5,
        out_specs=(vm,) * 2,
        compiler_params=pltpu.CompilerParams(vmem_limit_bytes=4 * 1024 * 1024),
        cost_estimate=pl.CostEstimate(flops=300_000_000, bytes_accessed=400_000, transcendentals=0),
        name="finish",
    )(tau8, rit, uit, u, li)


def gather_kernel(at_ref, a_v, pt_out, xh_out, xo_out, g_out, ptop_out, head_out,
                  pt_v, x_v, g_v, g_in, g_sum, g_end, x_in, head_v, ptop_v,
                  a_sem, own_sem, send, fwd, recv, h_sem, hsend, hrecv, psend, precv, gsend, grecv, xsend, xrecv):
    ncol, local_rows = at_ref.shape
    nch = local_rows // CH
    half = ncol // 2
    q = lax.axis_index('col')
    r = lax.axis_index('row')
    last = lax.axis_size('col') - 1

    def own_load(c):
        return pltpu.make_async_copy(at_ref.at[pl.ds(0, BW), pl.ds(c * CH, CH)], pt_v.at[c, q], own_sem.at[c])

    def a_load(c):
        return pltpu.make_async_copy(at_ref.at[:, pl.ds(c * CH, CH)], a_v.at[c], a_sem.at[c])

    def hop(c, j, to, sem):
        return pltpu.make_async_remote_copy(
            src_ref=pt_v.at[c, j], dst_ref=pt_v.at[c, j], send_sem=sem, recv_sem=recv.at[c, j],
            device_id={'col': to}, device_id_type=MESH)

    at_end = jnp.logical_or(q == 0, q == last)
    inward = jnp.where(q == 0, 1, -1)
    routes = ((q + 2 * inward, at_end, 0), (q + inward, at_end, 1), (q + 1, jnp.logical_not(at_end), 0), (q - 1, jnp.logical_not(at_end), 1))

    def send_own(c):
        own_load(c).wait()
        for to, valid, slot in routes:
            @pl.when(valid)
            def _():
                hop(c, q, to, send.at[c, slot]).start()

    def head_send(p):
        return pltpu.make_async_remote_copy(
            src_ref=at_ref.at[:, pl.ds(0, NC)], dst_ref=head_v, send_sem=hsend.at[p], recv_sem=hrecv,
            device_id={'row': p}, device_id_type=MESH)

    def ptop_send(p):
        return pltpu.make_async_remote_copy(
            src_ref=pt_v.at[0, :, :, pl.ds(0, NC)], dst_ref=ptop_v, send_sem=psend.at[p], recv_sem=precv,
            device_id={'row': p}, device_id_type=MESH)

    for c in range(nch):
        own_load(c).start()
    for c in range(nch):
        a_load(c).start()

    barrier = pltpu.get_barrier_semaphore()

    for to, valid in ((q + 2, q + 2 <= last), (q - 2, q >= 2), (q + 1, q < last), (q - 1, q > 0)):
        @pl.when(valid)
        def _():
            pl.semaphore_signal(barrier, inc=1, device_id={'col': to}, device_id_type=MESH)

    for d in range(1, 4):
        pl.semaphore_signal(barrier, inc=1, device_id={'row': (r + d) % 4}, device_id_type=MESH)
    inner = jnp.logical_not(at_end)
    outward = jnp.where(q == 1, -1, 1)

    @pl.when(inner)
    def _():
        pl.semaphore_wait(barrier, 6)

    @pl.when(jnp.logical_not(inner))
    def _():
        pl.semaphore_wait(barrier, 5)

    for c in range(nch):
        send_own(c)

    head_local = pltpu.make_async_copy(at_ref.at[:, pl.ds(0, NC)], head_v, h_sem)

    @pl.when(r == 0)
    def _():
        for p in range(1, 4):
            head_send(p).start()
        head_local.start()

    x_v[...] = jnp.zeros_like(x_v)
    g_v[...] = jnp.zeros_like(g_v)

    g_copies = []
    for d in range(1, 4):
        g_copies.append(pltpu.make_async_remote_copy(
            src_ref=g_v, dst_ref=g_in.at[d - 1], send_sem=gsend.at[d - 1], recv_sem=grecv.at[d - 1],
            device_id={'row': (r + d) % 4}, device_id_type=MESH))

    def chunk(c, carry):
        near, far = q - outward, q - 2 * outward

        @pl.when(inner)
        def _():
            hop(c, near, q, fwd.at[c, 0]).wait_recv()
            hop(c, near, q + outward, fwd.at[c, 0]).start()
            hop(c, far, q, fwd.at[c, 1]).wait_recv()
            hop(c, far, q + outward, fwd.at[c, 1]).start()
            hop(c, q + outward, q, fwd.at[c, 0]).wait_recv()

        @pl.when(at_end)
        def _():
            for d in range(1, 4):
                hop(c, q + d * inward, q, fwd.at[c, 0]).wait_recv()

        pt_out[c] = pt_v[c]

        @pl.when(jnp.logical_and(c == 0, r == 0))
        def _():
            for p in range(1, 4):
                ptop_send(p).start()
            for j in range(PANELS):
                ptop_out[j * BW:(j + 1) * BW, :] = pt_v[0, j, :, 0:NC]

        a_load(c).wait()
        p = pt_v[c].reshape(NC, CH)
        @pl.when(inner)
        def _():
            g_v[...] += dot_nt(p, p)

        @pl.when(jnp.logical_and(c == nch - 1, inner))
        def _():
            for g_copy in g_copies:
                g_copy.start()

        ah, am, al = split3(a_v[c])
        ph, pm, plo = split3(p)
        both = jnp.concatenate([ph, pm], axis=0)
        main = dot16_nt(ah, both) + dot16_nt(am, both)
        low = dot16_nt(jnp.concatenate([ah, al], axis=1), jnp.concatenate([plo, ph], axis=1))
        x_v[...] += main[:, 0:NC] + (main[:, NC:] + low)
        return carry

    lax.fori_loop(0, nch, chunk, 0)

    core = r % 2
    mate = r + 1 - 2 * core
    x_copy = pltpu.make_async_remote_copy(
        src_ref=x_v, dst_ref=x_in, send_sem=xsend, recv_sem=xrecv,
        device_id={'row': mate}, device_id_type=MESH)
    x_copy.start()

    part = pl.ds((NC // 2) * core, NC // 2)

    def half_copy(to):
        return pltpu.make_async_remote_copy(
            src_ref=g_sum.at[part], dst_ref=g_end.at[part], send_sem=gsend.at[3], recv_sem=grecv.at[3],
            device_id={'col': to}, device_id_type=MESH)

    mate_copy = pltpu.make_async_remote_copy(
        src_ref=g_end.at[part], dst_ref=g_end.at[part], send_sem=gsend.at[4], recv_sem=grecv.at[4],
        device_id={'row': mate}, device_id_type=MESH)
    @pl.when(r == 0)
    def _():
        for p in range(1, 4):
            head_send(p).wait_send()
            ptop_send(p).wait_send()
        head_local.wait()

    @pl.when(r > 0)
    def _():
        head_send(0).wait_recv()
        ptop_send(0).wait_recv()
        for j in range(PANELS):
            ptop_out[j * BW:(j + 1) * BW, :] = ptop_v[j]

    head_out[...] = head_v[...]

    def drain(c, carry):
        for to, valid, slot in routes:
            @pl.when(valid)
            def _():
                hop(c, q, to, send.at[c, slot]).wait_send()

        @pl.when(inner)
        def _():
            for slot in range(2):
                hop(c, q, q, fwd.at[c, slot]).wait_send()

        return carry

    lax.fori_loop(0, nch, drain, 0)
    @pl.when(inner)
    def _():
        for g_copy in g_copies:
            g_copy.wait()
        parts = [g_v[...]] + [g_in[d - 1] for d in range(1, 4)]
        total = None
        for row in range(4):
            dist = (r - row + 4) % 4
            part = jnp.where(dist == 0, parts[0], jnp.where(dist == 1, parts[1], jnp.where(dist == 2, parts[2], parts[3])))
            total = part if total is None else total + part
        g_out[...] = total
        g_sum[...] = total

    @pl.when(at_end)
    def _():
        half_copy(q).wait_recv()
        mate_copy.start()

    x_copy.wait()
    mine, other = pl.ds(half * core, half), pl.ds(half * (1 - core), half)
    xh_out[...] = x_v[mine, :] + x_in[mine, :]
    xo_out[...] = x_v[other, :] + x_in[other, :]

    @pl.when(inner)
    def _():
        half_copy(q + outward).start()
        half_copy(q + outward).wait_send()

    @pl.when(at_end)
    def _():
        mate_copy.wait()
        g_out[...] = g_end[...]


def gather(at):
    ncol, local_rows = at.shape
    nch = local_rows // CH
    f32 = jnp.float32
    vm, anys = pl.BlockSpec(memory_space=pltpu.VMEM), pl.BlockSpec(memory_space=pl.ANY)
    dma = pltpu.SemaphoreType.DMA
    return pl.pallas_call(
        gather_kernel,
        out_shape=(jax.ShapeDtypeStruct((nch, ncol, CH), f32), jax.ShapeDtypeStruct((nch, PANELS, BW, CH), f32), jax.ShapeDtypeStruct((ncol // 2, NC), f32), jax.ShapeDtypeStruct((ncol // 2, NC), f32),
                   jax.ShapeDtypeStruct((NC, NC), f32), jax.ShapeDtypeStruct((NC, NC), f32), jax.ShapeDtypeStruct((ncol, NC), f32)),
        in_specs=[anys],
        out_specs=(vm,) * 7,
        scratch_shapes=[pltpu.VMEM((nch, PANELS, BW, CH), f32), pltpu.VMEM((ncol, NC), f32),
                        pltpu.VMEM((NC, NC), f32), pltpu.VMEM((3, NC, NC), f32), pltpu.VMEM((NC, NC), f32), pltpu.VMEM((NC, NC), f32), pltpu.VMEM((ncol, NC), f32),
                        pltpu.VMEM((ncol, NC), f32), pltpu.VMEM((PANELS, BW, NC), f32),
                        dma((nch,)), dma((nch,)), dma((nch, 2)), dma((nch, 2)), dma((nch, 4)), dma, dma((4,)), dma, dma((4,)), dma,
                        dma((5,)), dma((5,)), dma, dma],
        compiler_params=pltpu.CompilerParams(collective_id=0, has_side_effects=True, vmem_limit_bytes=GATHER_VMEM),
        name="gather",
    )(at)


def update_kernel(a_ref, pt_ref, x0_ref, x1_ref, x2_ref, x3_ref, head_ref, rit_ref, nmat_ref, uit_ref, facet_ref, out_ref, z_v, top_v, sem, *strips):
    q = lax.axis_index('col')
    r = lax.axis_index('row')
    ncol = head_ref.shape[0]
    half = ncol // 2
    core = r % 2
    rit = rit_ref[...]
    nmat = nmat_ref[...]
    mine = pl.multiple_of(half * core, half)
    other = pl.multiple_of(half * (1 - core), half)
    for lo, xa, xb in ((mine, x0_ref, x1_ref), (other, x2_ref, x3_ref)):
        r12t = dot6(xa[...] + xb[...], rit, (1, 1))
        top_v[pl.ds(lo, half), :] = r12t
        z_v[pl.ds(lo, half), :] = stack6(dot6(head_ref[pl.ds(lo, half), :] - r12t, nmat, (1, 0)), 1, LEFT)
    own = pl.ds(pl.multiple_of(q * BW, BW), BW)
    top_v[0:BW, :] = facet_ref[own, :]
    z_v[0:BW, :] = stack6(-uit_ref[own, :], 1, LEFT)

    copies = []
    for step, strip in enumerate(strips):
        wide = [stack6(pt_ref[step * WIDE + i].reshape(NC, CH), 0, RIGHT) for i in range(WIDE)]
        parts = 4 if step == len(strips) - 1 else 2
        size = ncol // parts
        for part in range(parts):
            lo = part * size
            for i in range(WIDE):
                prod = lax.dot_general(z_v[lo:lo + size, :], wide[i], (((1,), (0,)), ((), ())), preferred_element_type=jnp.float32)
                src = step * WIDE + i
                if part == 0:
                    new = jnp.concatenate([-prod[0:BW], a_ref[src, BW:size, :] - prod[BW:]], axis=0)
                else:
                    new = a_ref[src, lo:lo + size, :] - prod
                if src == 0:
                    strip[lo:lo + size, 0:NC] = jnp.where(r == 0, top_v[lo:lo + size, :], new[:, 0:NC])
                    strip[lo:lo + size, NC:CH] = new[:, NC:]
                else:
                    strip[lo:lo + size, i * CH:(i + 1) * CH] = new
            copies.append(pltpu.make_async_copy(
                strip.at[pl.ds(lo, size)], out_ref.at[pl.ds(lo, size), pl.ds(step * WIDE * CH, WIDE * CH)], sem.at[len(copies)]))
            copies[-1].start()
    for copy in copies:
        copy.wait()


def update(a, pt, xs, head, rit, nmat, uit, facet):
    nch, ncol, _ = a.shape
    vm = pl.BlockSpec(memory_space=pltpu.VMEM)
    return pl.pallas_call(
        update_kernel,
        out_shape=jax.ShapeDtypeStruct((ncol, nch * CH), jnp.float32),
        in_specs=[vm] * 11,
        out_specs=pl.BlockSpec(memory_space=pl.ANY),
        scratch_shapes=[pltpu.VMEM((ncol, 6 * NC), jnp.bfloat16), pltpu.VMEM((ncol, NC), jnp.float32), pltpu.SemaphoreType.DMA((2 * nch,))]
        + [pltpu.VMEM((ncol, WIDE * CH), jnp.float32)] * (nch // WIDE),
        compiler_params=pltpu.CompilerParams(vmem_limit_bytes=UPDATE_VMEM),
        name="update",
    )(a, pt, *xs, head, rit, nmat, uit, facet)


def solution(mesh):
    block_spec = P(('batch', 'row'), 'col', None)

    def device_fn(a_local):
        local_rows, local_blocks, bw = a_local.shape
        ncol = local_blocks * bw
        at = a_local.transpose(1, 2, 0).reshape(ncol, local_rows)
        a, pt, xh, xo, gram, ptop, head = gather(at)
        x1 = lax.ppermute(xh, 'row', [(i, i ^ 2) for i in range(4)])
        facet, tau, tau8, rit, uit, u, li = factor(gram, ptop)
        x1, u = lax.optimization_barrier((x1, u))
        x3 = lax.ppermute(x1, 'row', [(i, i ^ 1) for i in range(4)])
        tfac, nmat = finish(tau8, rit, uit, u, li)
        out = update(a, pt, (xh, x1, xo, x3), head, rit, nmat, uit, facet)
        a_out = out.reshape(local_blocks, bw, local_rows).transpose(2, 0, 1)
        return a_out, tau.reshape(NC), tfac

    return jax.shard_map(device_fn, mesh=mesh, in_specs=(block_spec,), out_specs=(block_spec, P('batch'), P('batch', None, None)), check_vma=False)
```
